32 devices in a mesh: rep: 4 (over x, y), dp: 8 (over z, core).
Axes of the slice: x: 2, y: 2, z: 4, core: 2. Of those that a mesh axis runs over, the one named last changes fastest.
Arguments:
- x: bfloat16 [32, 2048, 640], P(('rep', 'dp')), parts along dimension 0
- dy: bfloat16 [32, 2048, 640], P(('rep', 'dp')), parts along dimension 0
- w_gate: bfloat16 [2, 640, 2432], replicated
- w_up: bfloat16 [2, 640, 2432], replicated
- w_down: bfloat16 [2, 2432, 640], replicated
- m_w_gate: float32 [2, 640, 2432], replicated
- m_w_up: float32 [2, 640, 2432], replicated
- m_w_down: float32 [2, 2432, 640], replicated
- v_w_gate: float32 [2, 640, 2432], replicated
- v_w_up: float32 [2, 640, 2432], replicated
- v_w_down: float32 [2, 2432, 640], replicated
Outputs:
- output 1: bfloat16 [8, 640, 2432], P('rep'), parts along dimension 0
- output 2: bfloat16 [8, 640, 2432], P('rep'), parts along dimension 0
- output 3: bfloat16 [8, 2432, 640], P('rep'), parts along dimension 0
- output 4: float32 [8, 640, 2432], P('rep'), parts along dimension 0
- output 5: float32 [8, 640, 2432], P('rep'), parts along dimension 0
- output 6: float32 [8, 2432, 640], P('rep'), parts along dimension 0
- output 7: float32 [8, 640, 2432], P('rep'), parts along dimension 0
- output 8: float32 [8, 640, 2432], P('rep'), parts along dimension 0
- output 9: float32 [8, 2432, 640], P('rep'), parts along dimension 0
There are 4 independent parts. The reference program is written for one: setup_inputs(seed, part) draws one part's arguments, and reference() takes and returns one part's arrays. A program takes and returns all parts, laid end to end along the dimension named above; an argument that names none is the same for every part.
All inputs are finite; a program needn't handle non-finite values.
Results may differ from the reference program's by a relative error of at most 0.022.
Values are sent between devices in bfloat16 or wider.
A program may use at most 2.5 GiB of HBM per device.

```python
import jax
import jax.numpy as jnp
from jax import lax

SEQUENCES = 8
TOKENS = 2048
D = 640
FF = 2432
LAYERS = 2
NAMES = ("w_gate", "w_up", "w_down")
SHAPES = {"w_gate": (LAYERS, D, FF), "w_up": (LAYERS, D, FF), "w_down": (LAYERS, FF, D)}


def bump(key, n, height):
    away = (jnp.arange(n, dtype=jnp.int32) - jax.random.randint(key, (), 0, n, jnp.int32)) % n
    return jnp.where(away < n // 8, height, 1.0)


def together(key, own, strength):
    shared = jax.random.normal(key, own.shape[1:], jnp.float32)
    return (own + strength * shared) * lax.rsqrt(1 + strength * strength)


def setup_inputs(seed: int = 0, part: int = 0) -> dict:
    kx, kdy, ka, kb, kz, kf, kh, kl, *keys = jax.random.split(jax.random.key(seed), 8 + 3 * len(NAMES))
    kx, kdy, ka, kb = (jax.random.fold_in(k, part) for k in (kx, kdy, ka, kb))
    kw, km, kv = (keys[i::3] for i in range(3))
    shape = (SEQUENCES, TOKENS, D)
    much_x, much_dy = jax.random.uniform(kz, (2,), jnp.float32, 0.0, 1.0)
    loud = 2.0 ** jax.random.uniform(jax.random.fold_in(kz, 1), (), jnp.float32, -1.0, 2.0)
    layers = 2.0 ** jax.random.uniform(kl, (LAYERS, 1, 1), jnp.float32, -1.0, 1.0)
    x = together(ka, jax.random.normal(kx, shape, jnp.float32), much_x) * bump(kf, D, 4.0)
    dy = together(kb, jax.random.normal(kdy, shape, jnp.float32), much_dy)
    drawn = {"x": x.astype(jnp.bfloat16), "dy": (loud * dy * (SEQUENCES * TOKENS) ** -0.5).astype(jnp.bfloat16)}
    for key, name in zip(kw, NAMES, strict=True):
        w = jax.random.normal(key, SHAPES[name], jnp.float32) * SHAPES[name][1] ** -0.5
        drawn[name] = (w * {"w_gate": 1.0, "w_up": bump(kh, FF, 4.0), "w_down": layers}[name]).astype(jnp.bfloat16)
    for key, name in zip(km, NAMES, strict=True):
        drawn[f"m_{name}"] = 0.1 * jax.random.normal(key, SHAPES[name], jnp.float32)
    for key, name in zip(kv, NAMES, strict=True):
        drawn[f"v_{name}"] = jax.random.uniform(key, SHAPES[name], jnp.float32, 0.005, 0.015)
    return drawn


def matmul(a, w):
    return jnp.dot(a, w, preferred_element_type=jnp.float32).astype(jnp.bfloat16)


def normed(h):
    wide = h.astype(jnp.float32)
    scale = lax.rsqrt(jnp.mean(wide**2, -1, keepdims=True) + 1e-6)
    return (wide * scale).astype(jnp.bfloat16)


def layer(h, w):
    a = normed(h)
    gate = jnp.dot(a, w["w_gate"], preferred_element_type=jnp.float32)
    up = jnp.dot(a, w["w_up"], preferred_element_type=jnp.float32)
    return h + matmul((jax.nn.silu(gate) * up).astype(jnp.bfloat16), w["w_down"])


def adamw(w, m, v, g):
    m = 0.9 * m + 0.1 * g
    v = 0.95 * v + 0.05 * g * g
    step = m * lax.rsqrt(v + 1e-8) + 0.1 * w
    return (w - 0.02 * step).astype(jnp.bfloat16), m, v


def clipped(gradients, sum_of_squares, count):
    factor = jnp.minimum(1.0, 0.5 * lax.rsqrt(sum_of_squares / count + 1e-30))
    return [g * factor for g in gradients]


def stack(weights, h):
    return lax.scan(lambda h, w: (layer(h, w), None), h, weights)[0]


def reference(x, dy, w_gate, w_up, w_down, m_w_gate, m_w_up, m_w_down, v_w_gate, v_w_up, v_w_down):
    weights = dict(zip(NAMES, (w_gate, w_up, w_down), strict=True))

    def take(so_far, sequence):
        h, by_y = sequence
        _, back = jax.vjp(lambda w: stack(w, h), weights)
        return jax.tree.map(lambda total, term: total + term.astype(jnp.float32), so_far, back(by_y)[0]), None

    none_yet = {name: jnp.zeros(w.shape, jnp.float32) for name, w in weights.items()}
    by_weights, _ = lax.scan(take, none_yet, (x, dy))
    gradients = [by_weights[name].astype(jnp.bfloat16).astype(jnp.float32) for name in NAMES]
    gradients = clipped(gradients, sum(jnp.sum(g * g) for g in gradients), sum(g.size for g in gradients))
    new = [
        adamw(w.astype(jnp.float32), m, v, g)
        for w, m, v, g in zip((w_gate, w_up, w_down), (m_w_gate, m_w_up, m_w_down), (v_w_gate, v_w_up, v_w_down), gradients, strict=True)
    ]
    return tuple(one[which] for which in range(3) for one in new)
```

```python
import functools

import jax
import jax.numpy as jnp
from jax import lax
from jax.experimental import pallas as pl
from jax.experimental.pallas import tpu as pltpu
from jax.sharding import PartitionSpec as P

F32, BF16 = jnp.float32, jnp.bfloat16
MESH = pl.DeviceIdType.MESH
T, D, FF = 2048, 640, 2432
TILE = 256
STEPS = 10
LANES = 128
PER_LAYER = FF // LANES
UNITS = 2 * PER_LAYER
ROWS = 512
HALF, QUARTER = D // 2, D // 4
KEEP = 10
SLOTS = 4
LAG = 2
LAST = 2 * 2 * STEPS + 2 + 3 * LAG


def dot(a, b):
    return jnp.dot(a, b, preferred_element_type=F32)


def dot_t(a, b):
    return lax.dot_general(a, b, (((1,), (1,)), ((), ())), preferred_element_type=F32)


def norm_scale(h):
    wide = h.astype(F32)
    return wide, lax.rsqrt(jnp.mean(wide * wide, -1, keepdims=True) + 1e-6)


def gradient_kernel(
    x_hbm, dy_hbm, wg_hbm, wu_hbm, wd_hbm, g_hbm, ss_out,
    X, A, AT, H, DY, DYT, ACC, DT, ACT, WGU, WD, OWN, PART, UP, OUT, SQ, SS,
    sem_in, sem_w, sem_d2d, sem_part, sem_up, sem_out, sem_g, sem_gsend, sem_gd2d, sem_gpart, sem_ss, sem_sssend,
):
    rep, dp = lax.axis_index("rep"), lax.axis_index("dp")
    z, core = lax.div(dp, 2), lax.rem(dp, 2)

    def at(z, core):
        return (rep, z * 2 + core)

    partner = at(z, 1 - core)
    barrier = pltpu.get_barrier_semaphore()
    for other in range(1, 8):
        pl.semaphore_signal(barrier, inc=1, device_id=(rep, lax.rem(dp + other, 8)), device_id_type=MESH)

    x_copy = pltpu.make_async_copy(x_hbm.at[0], X, sem_in.at[0])
    dy_copy = pltpu.make_async_copy(dy_hbm.at[0], DY, sem_in.at[1])
    x_copy.start()

    def tile_copies(q, n):
        layer = jnp.where((q >= STEPS) & (q < 2 * STEPS), 1, 0)
        slot = lax.rem(q, 2)
        columns = pl.ds(pl.multiple_of(lax.rem(q, STEPS) * TILE, LANES), n)
        return (
            pltpu.make_async_copy(wg_hbm.at[layer, :, columns], WGU.at[slot, :, pl.ds(0, n)], sem_w.at[slot, 0]),
            pltpu.make_async_copy(wu_hbm.at[layer, :, columns], WGU.at[slot, :, pl.ds(TILE, n)], sem_w.at[slot, 1]),
            pltpu.make_async_copy(wd_hbm.at[layer, columns, :], WD.at[slot, pl.ds(0, n), :], sem_w.at[slot, 2]),
        )

    def load(q):
        short = lax.rem(q, STEPS) == STEPS - 1
        slot = lax.rem(q, 2)

        @pl.when(jnp.logical_not(short))
        def _():
            for copy in tile_copies(q, TILE):
                copy.start()

        @pl.when(short)
        def _():
            WGU[slot, :, LANES:TILE] = jnp.zeros((D, LANES), BF16)
            WGU[slot, :, TILE + LANES :] = jnp.zeros((D, LANES), BF16)
            WD[slot, LANES:, :] = jnp.zeros((LANES, D), BF16)
            for copy in tile_copies(q, LANES):
                copy.start()

    def wait_tile(q):
        short = lax.rem(q, STEPS) == STEPS - 1

        @pl.when(jnp.logical_not(short))
        def _():
            for copy in tile_copies(q, TILE):
                copy.wait()

        @pl.when(short)
        def _():
            for copy in tile_copies(q, LANES):
                copy.wait()

    load(jnp.int32(0))
    dy_copy.start()
    x_copy.wait()
    block = 256

    def rows_of(r):
        return pl.ds(pl.multiple_of(r * block, block), block)

    @pl.loop(0, T // block)
    def _(r):
        rows = rows_of(r)
        wide, scale = norm_scale(X[rows, :])
        A[rows, :] = (wide * scale).astype(BF16)

    def forward(q, first):
        slot = lax.rem(q, 2)
        wait_tile(q)
        load(q + 1)
        for r in range(0, T, ROWS):
            gu = dot(A[r : r + ROWS, :], WGU[slot])
            g, u = gu[:, :TILE], gu[:, TILE:]
            sig = 0.5 * jnp.tanh(0.5 * g) + 0.5
            h = dot((g * sig * u).astype(BF16), WD[slot])
            if first:
                ACC[r : r + ROWS, :] = h
            else:
                ACC[r : r + ROWS, :] += h

    forward(jnp.int32(0), True)

    @pl.loop(1, STEPS)
    def _(q):
        forward(q, False)

    dy_copy.wait()

    @pl.loop(0, T // block)
    def _(r):
        rows = rows_of(r)
        h = (X[rows, :].astype(F32) + ACC[rows, :].astype(BF16).astype(F32)).astype(BF16)
        H[rows, :] = h
        wide, scale = norm_scale(h)
        a = (wide * scale).astype(BF16)
        A[rows, :] = a
        AT[:, rows] = a.T
        DYT[:, rows] = DY[rows, :].T

    pl.semaphore_wait(barrier, 7)

    def next_layer():
        @pl.loop(0, T // block)
        def _(r):
            rows = rows_of(r)
            h, scale = norm_scale(H[rows, :])
            da = ACC[rows, :].astype(BF16).astype(F32)
            along = jnp.mean(da * h, -1, keepdims=True) * scale * scale
            dh = (scale * (da - h * along)).astype(BF16)
            d = (DY[rows, :].astype(F32) + dh.astype(F32)).astype(BF16)
            DY[rows, :] = d
            DYT[:, rows] = d.T
            wide, scale = norm_scale(X[rows, :])
            a = (wide * scale).astype(BF16)
            A[rows, :] = a
            AT[:, rows] = a.T

    SQ[...] = jnp.zeros_like(SQ)

    def exists(v):
        return (v >= 0) & (v < 4 * STEPS) & (lax.rem(v, 2 * STEPS) != 2 * STEPS - 1)

    def packed(v):
        return v - jnp.where(v >= 2 * STEPS, 1, 0)

    def part_copy(v):
        w = packed(v)
        return pltpu.make_async_remote_copy(
            src_ref=OWN.at[lax.rem(v, KEEP), :, pl.ds(pl.multiple_of((1 - core) * HALF, 16), HALF), :],
            dst_ref=PART.at[w],
            send_sem=sem_d2d.at[lax.rem(v, 4)],
            recv_sem=sem_part.at[w],
            device_id=partner,
            device_id_type=MESH,
        )

    def my_rows(way):
        return pl.ds(pl.multiple_of(core * HALF + way * QUARTER, 16), QUARTER)

    def up_copy(way, w):
        return pltpu.make_async_remote_copy(
            src_ref=OUT.at[way, lax.rem(w, SLOTS)],
            dst_ref=UP.at[way, w],
            send_sem=sem_out.at[way, lax.rem(w, SLOTS)],
            recv_sem=sem_up.at[way, w],
            device_id=at(jnp.clip(z - 1, 0, 3) if way == 0 else jnp.clip(z + 1, 0, 3), core),
            device_id_type=MESH,
        )

    def keep_copy(way, w):
        return pltpu.make_async_copy(
            OUT.at[way, lax.rem(w, SLOTS)], g_hbm.at[w, :, my_rows(way), :], sem_out.at[way, lax.rem(w, SLOTS)]
        )

    def reduce(way, v):
        starts, ends = (z == 3, z == 0) if way == 0 else (z == 0, z == 3)
        comes_first = (z >= 2) if way == 0 else (z < 2)

        @pl.when(exists(v))
        def _():
            w = packed(v)
            slot = lax.rem(w, SLOTS)

            @pl.when(comes_first)
            def _():
                part_copy(v).wait_recv()

            @pl.when(w >= SLOTS)
            def _():
                keep_copy(way, w).wait()

            rows = pl.ds(way * QUARTER, QUARTER)

            def two(k):
                own = OWN[lax.rem(v, KEEP), k, my_rows(way), :].astype(F32)
                return own + PART[w, k, rows, :].astype(F32)

            @pl.when(starts)
            def _():
                for k in range(3):
                    OUT[way, slot, k] = two(k).astype(BF16)

            @pl.when(jnp.logical_not(starts))
            def _():
                up_copy(way, w).wait_recv()
                for k in range(3):
                    OUT[way, slot, k] = (two(k) + UP[way, w, k].astype(F32)).astype(BF16)

            @pl.when(jnp.logical_not(ends))
            def _():
                up_copy(way, w).start()

            @pl.when(ends)
            def _():
                keep_copy(way, w).start()
                total = jnp.zeros((8, LANES), F32)
                for k in range(3):
                    g = OUT[way, slot, k].astype(F32)
                    total += jnp.sum((g * g).reshape(QUARTER // 8, 8, LANES), 0)
                SQ[...] += total

    def communicate(n):
        reduce(0, n - 2 - LAG * (3 - z))
        reduce(1, n - 2 - LAG * z)

    @pl.loop(0, 2 * STEPS)
    def _(t):
        q = t + STEPS
        slot = lax.rem(q, 2)

        @pl.when(t == STEPS)
        def _():
            next_layer()

        wait_tile(q)

        @pl.when(q < 3 * STEPS - 1)
        def _():
            load(q + 1)

        for r in range(0, T, ROWS):
            gu = dot(A[r : r + ROWS, :], WGU[slot])
            da = dot_t(DY[r : r + ROWS, :], WD[slot]).astype(BF16).astype(F32)
            g, u = gu[:, :TILE], gu[:, TILE:]
            sig = 0.5 * jnp.tanh(0.5 * g) + 0.5
            s = g * sig
            ACT[r : r + ROWS, :] = (s * u).astype(BF16)
            DT[r : r + ROWS, TILE:] = (da * s).astype(BF16)
            DT[r : r + ROWS, :TILE] = (da * u * (sig + s * (1.0 - sig))).astype(BF16)

        communicate(2 * t)

        keep = lax.rem(t, KEEP // 2) * 2
        dgu = dot(AT[...], DT[...]).astype(BF16)
        for k in range(2):
            for half in range(2):
                OWN[keep + half, k] = dgu[:, k * TILE + half * LANES : k * TILE + (half + 1) * LANES]
        dd = dot(DYT[...], ACT[...]).astype(BF16)
        for half in range(2):
            OWN[keep + half, 2] = dd[:, half * LANES : (half + 1) * LANES]

        for half in range(2):
            v = 2 * t + half

            @pl.when(exists(v - 2))
            def _():
                part_copy(v - 2).wait_send()

            @pl.when(exists(v))
            def _():
                part_copy(v).start()

        @pl.when(t == 0)
        def _():
            ACC[...] = jnp.zeros_like(ACC)

        @pl.when(t < STEPS)
        def _():
            for r in range(0, T, ROWS):
                ACC[r : r + ROWS, :] += dot_t(DT[r : r + ROWS, :], WGU[slot])

        communicate(2 * t + 1)

    part_copy(jnp.int32(4 * STEPS - 2)).wait_send()

    @pl.loop(4 * STEPS, LAST)
    def _(n):
        communicate(n)

    for way in range(2):
        for w in range(UNITS - SLOTS, UNITS):
            keep_copy(way, jnp.int32(w)).wait()

    mine = jnp.where(z == 3, 2, 0) + core
    holds = (z == 0) | (z == 3)

    def ss_copy(other):
        return pltpu.make_async_remote_copy(
            src_ref=SQ,
            dst_ref=SS.at[mine],
            send_sem=sem_sssend.at[other],
            recv_sem=sem_ss.at[mine],
            device_id=(rep, lax.rem(dp + other, 8)),
            device_id_type=MESH,
        )

    @pl.when(holds)
    def _():
        for other in range(1, 8):
            ss_copy(other).start()
        SS[mine] = SQ[...]

    def g_rows(way, w):
        return g_hbm.at[w, :, my_rows(way), :]

    def forward_copy(way, w):
        return pltpu.make_async_remote_copy(
            src_ref=g_rows(way, w),
            dst_ref=g_rows(way, w),
            send_sem=sem_gsend.at[way],
            recv_sem=sem_g.at[way, w],
            device_id=at(jnp.clip(z + 1, 0, 3) if way == 0 else jnp.clip(z - 1, 0, 3), core),
            device_id_type=MESH,
        )

    def share_copy(way, w):
        return pltpu.make_async_remote_copy(
            src_ref=g_rows(way, w),
            dst_ref=g_rows(way, w),
            send_sem=sem_gd2d.at[way],
            recv_sem=sem_gpart.at[way],
            device_id=partner,
            device_id_type=MESH,
        )

    @pl.loop(0, UNITS + 6)
    def _(n):
        for way in range(2):
            distance = z if way == 0 else 3 - z
            w = n - 2 * distance

            @pl.when((w >= 0) & (w < UNITS))
            def _():
                @pl.when(distance > 0)
                def _():
                    forward_copy(way, w).wait_recv()

                @pl.when(distance < 3)
                def _():
                    forward_copy(way, w).start()

                share_copy(way, w).start()

    for way in range(2):
        theirs = pl.ds(pl.multiple_of((1 - core) * HALF + way * QUARTER, 16), QUARTER)
        everything = g_hbm.at[:, :, my_rows(way), :]
        others = g_hbm.at[:, :, theirs, :]

        @pl.when((z < 3) if way == 0 else (z > 0))
        def _():
            pltpu.make_async_copy(everything, everything, sem_gsend.at[way]).wait()

        pltpu.make_async_copy(everything, everything, sem_gd2d.at[way]).wait()
        pltpu.make_async_copy(others, others, sem_gpart.at[way]).wait()

    for piece in range(4):

        @pl.when(jnp.logical_not(holds & (mine == piece)))
        def _():
            pltpu.make_async_copy(SS.at[piece], SS.at[piece], sem_ss.at[piece]).wait()

    @pl.when(holds)
    def _():
        for other in range(1, 8):
            ss_copy(other).wait_send()

    ss_out[...] = (SS[0] + SS[1]) + (SS[2] + SS[3])


def gradients(x, dy, w_gate, w_up, w_down):
    hbm = pl.BlockSpec(memory_space=pl.ANY)

    def vmem(*shape):
        return pltpu.VMEM(shape, BF16)

    dma = pltpu.SemaphoreType.DMA
    return pl.pallas_call(
        gradient_kernel,
        out_shape=(
            jax.ShapeDtypeStruct((UNITS, 3, D, LANES), BF16),
            jax.ShapeDtypeStruct((8, LANES), F32),
        ),
        in_specs=[hbm] * 5,
        out_specs=(hbm, pl.BlockSpec(memory_space=pltpu.VMEM)),
        scratch_shapes=[
            vmem(T, D), vmem(T, D), vmem(D, T), vmem(T, D), vmem(T, D), vmem(D, T),
            pltpu.VMEM((T, D), F32),
            vmem(T, 2 * TILE), vmem(T, TILE), vmem(2, D, 2 * TILE), vmem(2, TILE, D),
            vmem(KEEP, 3, D, LANES), vmem(UNITS, 3, HALF, LANES), vmem(2, UNITS, 3, QUARTER, LANES),
            vmem(2, SLOTS, 3, QUARTER, LANES),
            pltpu.VMEM((8, LANES), F32), pltpu.VMEM((4, 8, LANES), F32),
            dma((2,)), dma((2, 3)), dma((4,)), dma((UNITS,)), dma((2, UNITS)), dma((2, SLOTS)),
            dma((2, UNITS)), dma((2,)), dma((2,)), dma((2,)), dma((4,)), dma((8,)),
        ],
        compiler_params=pltpu.CompilerParams(collective_id=0, has_side_effects=True, vmem_limit_bytes=63 * 2**20),
        name="gradients",
    )(x, dy, w_gate, w_up, w_down)


def update(w, m, v, g):
    m = 0.9 * m + 0.1 * g
    v = 0.95 * v + 0.05 * g * g
    step = m * lax.rsqrt(v + 1e-8) + 0.1 * w
    return (w - 0.02 * step).astype(BF16), m, v


def clip_factor(ss_ref):
    total = jnp.sum(ss_ref[...], keepdims=True)
    return jnp.minimum(1.0, 0.5 * lax.rsqrt(total / (UNITS * 3 * D * LANES) + 1e-30))


def rows_kernel(ss, g, w, m, v, w_out, m_out, v_out):
    factor = clip_factor(ss)
    for unit in range(PER_LAYER):
        at = (0, slice(None), slice(unit * LANES, (unit + 1) * LANES))
        new = update(w[at].astype(F32), m[at], v[at], g[unit, 0].astype(F32) * factor)
        w_out[at], m_out[at], v_out[at] = new


def columns_kernel(ss, g, w, m, v, w_out, m_out, v_out):
    factor = clip_factor(ss)
    gradient = g[0, 0].astype(F32).T * factor
    w_out[0], m_out[0], v_out[0] = update(w[0].astype(F32), m[0], v[0], gradient)


def adamw(which, ss, g, w, m, v):
    if which < 2:
        rows = 64
        grid = (2, D // rows)
        kernel = rows_kernel
        g_spec = pl.BlockSpec((PER_LAYER, 1, rows, LANES), lambda layer, i: (1 - layer, which, i, 0))
        spec = pl.BlockSpec((1, rows, FF), lambda layer, i: (layer, i, 0))
    else:
        grid = (2, PER_LAYER)
        kernel = columns_kernel
        g_spec = pl.BlockSpec((1, 1, D, LANES), lambda layer, i: ((1 - layer) * PER_LAYER + i, 2, 0, 0))
        spec = pl.BlockSpec((1, LANES, D), lambda layer, i: (layer, i, 0))
    return pl.pallas_call(
        kernel,
        grid=grid,
        in_specs=[pl.BlockSpec((8, LANES), lambda layer, i: (0, 0)), g_spec, spec, spec, spec],
        out_specs=(spec, spec, spec),
        out_shape=(
            jax.ShapeDtypeStruct(w.shape, BF16),
            jax.ShapeDtypeStruct(w.shape, F32),
            jax.ShapeDtypeStruct(w.shape, F32),
        ),
        compiler_params=pltpu.CompilerParams(vmem_limit_bytes=48 * 2**20),
        name=f"adamw_{which}",
    )(ss, g, w, m, v)


def solution(mesh):
    def step(x, dy, *arrays):
        weights, m, v = (arrays[i : i + 3] for i in (0, 3, 6))
        g, ss = gradients(x, dy, *weights)
        new = [adamw(which, ss, g, weights[which], m[which], v[which]) for which in range(3)]
        return tuple(one[which] for which in range(3) for one in new)

    return jax.shard_map(
        step,
        mesh=mesh,
        in_specs=(P(("rep", "dp"), None, None),) * 2 + (P(None, None, None),) * 9,
        out_specs=(P("rep", None, None),) * 9,
        check_vma=False,
    )
```

```python
import functools

import jax
import jax.numpy as jnp
from jax import lax
from jax.experimental import pallas as pl
from jax.experimental.pallas import tpu as pltpu
from jax.sharding import PartitionSpec as P

F32, BF16 = jnp.float32, jnp.bfloat16
MESH = pl.DeviceIdType.MESH
T, D, FF = 2048, 640, 2432
TILE = 256
STEPS = 10
LANES = 128
PER_LAYER = FF // LANES
UNITS = 2 * PER_LAYER
ROWS = 512
HALF = D // 2
KEEP = 10
SLOTS = 4
LAG = 2
LAST = 2 * 2 * STEPS + 2 + 3 * LAG
EARLY, RATE = 14, 1

DEEP, AHEAD = 6, 3


def dot(a, b):
    return jnp.dot(a, b, preferred_element_type=F32)


def dot_t(a, b):
    return lax.dot_general(a, b, (((1,), (1,)), ((), ())), preferred_element_type=F32)


def norm_scale(h):
    wide = h.astype(F32)
    return wide, lax.rsqrt(jnp.mean(wide * wide, -1, keepdims=True) + 1e-6)


def gradient_kernel(
    x_hbm, dy_hbm, wg_hbm, wu_hbm, wd_hbm, g_hbm, ss_out,
    X, A, AT, H, DY, DYT, ACC, DT, ACT, WGU, WD, OWN, PART, UP, OUT, SQ, SS,
    sem_in, sem_w, sem_d2d, sem_part, sem_up, sem_out, sem_g, sem_gsend, sem_gd2d, sem_gpart, sem_ss, sem_sssend,
):
    rep, dp = lax.axis_index("rep"), lax.axis_index("dp")
    z, core = lax.div(dp, 2), lax.rem(dp, 2)

    def at(z, core):
        return (rep, z * 2 + core)

    partner = at(z, 1 - core)
    barrier = pltpu.get_barrier_semaphore()
    for other in range(1, 8):
        pl.semaphore_signal(barrier, inc=1, device_id=(rep, lax.rem(dp + other, 8)), device_id_type=MESH)

    x_copy = pltpu.make_async_copy(x_hbm.at[0], X, sem_in.at[0])
    dy_copy = pltpu.make_async_copy(dy_hbm.at[0], DY, sem_in.at[1])
    x_copy.start()

    def tile_copies(q, n):
        layer = jnp.where((q >= STEPS) & (q < 2 * STEPS), 1, 0)
        slot = lax.rem(q, 2)
        columns = pl.ds(pl.multiple_of(lax.rem(q, STEPS) * TILE, LANES), n)
        return (
            pltpu.make_async_copy(wg_hbm.at[layer, :, columns], WGU.at[slot, :, pl.ds(0, n)], sem_w.at[slot, 0]),
            pltpu.make_async_copy(wu_hbm.at[layer, :, columns], WGU.at[slot, :, pl.ds(TILE, n)], sem_w.at[slot, 1]),
            pltpu.make_async_copy(wd_hbm.at[layer, columns, :], WD.at[slot, pl.ds(0, n), :], sem_w.at[slot, 2]),
        )

    def load(q):
        short = lax.rem(q, STEPS) == STEPS - 1
        slot = lax.rem(q, 2)

        @pl.when(jnp.logical_not(short))
        def _():
            for copy in tile_copies(q, TILE):
                copy.start()

        @pl.when(short)
        def _():
            WGU[slot, :, LANES:TILE] = jnp.zeros((D, LANES), BF16)
            WGU[slot, :, TILE + LANES :] = jnp.zeros((D, LANES), BF16)
            WD[slot, LANES:, :] = jnp.zeros((LANES, D), BF16)
            for copy in tile_copies(q, LANES):
                copy.start()

    def wait_tile(q):
        short = lax.rem(q, STEPS) == STEPS - 1

        @pl.when(jnp.logical_not(short))
        def _():
            for copy in tile_copies(q, TILE):
                copy.wait()

        @pl.when(short)
        def _():
            for copy in tile_copies(q, LANES):
                copy.wait()

    load(jnp.int32(0))
    dy_copy.start()
    x_copy.wait()
    block = 256

    def rows_of(r):
        return pl.ds(pl.multiple_of(r * block, block), block)

    @pl.loop(0, T // block)
    def _(r):
        rows = rows_of(r)
        wide, scale = norm_scale(X[rows, :])
        A[rows, :] = (wide * scale).astype(BF16)

    def forward(q, first):
        slot = lax.rem(q, 2)
        wait_tile(q)
        load(q + 1)
        for r in range(0, T, ROWS):
            gu = dot(A[r : r + ROWS, :], WGU[slot])
            g, u = gu[:, :TILE], gu[:, TILE:]
            sig = 0.5 * jnp.tanh(0.5 * g) + 0.5
            h = dot((g * sig * u).astype(BF16), WD[slot])
            if first:
                ACC[r : r + ROWS, :] = h
            else:
                ACC[r : r + ROWS, :] += h

    forward(jnp.int32(0), True)

    @pl.loop(1, STEPS)
    def _(q):
        forward(q, False)

    dy_copy.wait()

    @pl.loop(0, T // block)
    def _(r):
        rows = rows_of(r)
        h = (X[rows, :].astype(F32) + ACC[rows, :].astype(BF16).astype(F32)).astype(BF16)
        H[rows, :] = h
        wide, scale = norm_scale(h)
        a = (wide * scale).astype(BF16)
        A[rows, :] = a
        AT[:, rows] = a.T
        DYT[:, rows] = DY[rows, :].T

    pl.semaphore_wait(barrier, 7)

    def next_layer():
        @pl.loop(0, T // block)
        def _(r):
            rows = rows_of(r)
            h, scale = norm_scale(H[rows, :])
            da = ACC[rows, :].astype(BF16).astype(F32)
            along = jnp.mean(da * h, -1, keepdims=True) * scale * scale
            dh = (scale * (da - h * along)).astype(BF16)
            d = (DY[rows, :].astype(F32) + dh.astype(F32)).astype(BF16)
            DY[rows, :] = d
            DYT[:, rows] = d.T
            wide, scale = norm_scale(X[rows, :])
            a = (wide * scale).astype(BF16)
            A[rows, :] = a
            AT[:, rows] = a.T

    SQ[...] = jnp.zeros_like(SQ)
    distance = jnp.where(core == 0, 3 - z, z)
    onward = jnp.where(core == 0, jnp.maximum(z - 1, 0), jnp.minimum(z + 1, 3))
    back = jnp.where(core == 0, jnp.minimum(z + 1, 3), jnp.maximum(z - 1, 0))
    mine = pl.ds(pl.multiple_of(core * HALF, 16), HALF)
    theirs = pl.ds(pl.multiple_of((1 - core) * HALF, 16), HALF)

    def exists(v):
        return (v >= 0) & (v < 4 * STEPS) & (lax.rem(v, 2 * STEPS) != 2 * STEPS - 1)

    def packed(v):
        return v - jnp.where(v >= 2 * STEPS, 1, 0)

    def part_copy(v):
        w = packed(v)
        return pltpu.make_async_remote_copy(
            src_ref=OWN.at[lax.rem(v, KEEP), :, theirs, :],
            dst_ref=PART.at[w],
            send_sem=sem_d2d.at[lax.rem(v, 4)],
            recv_sem=sem_part.at[w],
            device_id=partner,
            device_id_type=MESH,
        )

    def up_copy(w):
        return pltpu.make_async_remote_copy(
            src_ref=OUT.at[lax.rem(w, SLOTS)],
            dst_ref=UP.at[w],
            send_sem=sem_out.at[lax.rem(w, SLOTS)],
            recv_sem=sem_up.at[w],
            device_id=at(onward, core),
            device_id_type=MESH,
        )

    def keep_copy(w):
        return pltpu.make_async_copy(OUT.at[lax.rem(w, SLOTS)], g_hbm.at[w, :, mine, :], sem_out.at[lax.rem(w, SLOTS)])

    def reduce(v):
        @pl.when(exists(v))
        def _():
            w = packed(v)
            slot = lax.rem(w, SLOTS)
            part_copy(v).wait_recv()

            @pl.when(w >= SLOTS)
            def _():
                keep_copy(w).wait()

            def two(k):
                return OWN[lax.rem(v, KEEP), k, mine, :].astype(F32) + PART[w, k].astype(F32)

            @pl.when(distance == 0)
            def _():
                for k in range(3):
                    OUT[slot, k] = two(k).astype(BF16)

            @pl.when(distance > 0)
            def _():
                up_copy(w).wait_recv()
                for k in range(3):
                    OUT[slot, k] = (two(k) + UP[w, k].astype(F32)).astype(BF16)

            @pl.when(distance < 3)
            def _():
                up_copy(w).start()

            @pl.when(distance == 3)
            def _():
                keep_copy(w).start()
                total = jnp.zeros((8, LANES), F32)
                for k in range(3):
                    g = OUT[slot, k].astype(F32)
                    total += jnp.sum((g * g).reshape(HALF // 8, 8, LANES), 0)
                SQ[...] += total

    def back_copy(w):
        return pltpu.make_async_remote_copy(
            src_ref=g_hbm.at[w, :, mine, :],
            dst_ref=g_hbm.at[w, :, mine, :],
            send_sem=sem_gsend.at[0],
            recv_sem=sem_g.at[w],
            device_id=at(back, core),
            device_id_type=MESH,
        )

    def share_copy(w):
        return pltpu.make_async_remote_copy(
            src_ref=g_hbm.at[w, :, mine, :],
            dst_ref=g_hbm.at[w, :, mine, :],
            send_sem=sem_gd2d.at[0],
            recv_sem=sem_gpart.at[0],
            device_id=partner,
            device_id_type=MESH,
        )

    def gather(n):
        w = n - (3 - distance)

        @pl.when((w >= 0) & (w < UNITS))
        def _():
            @pl.when(distance < 3)
            def _():
                back_copy(w).wait_recv()

            @pl.when(distance > 0)
            def _():
                back_copy(w).start()

            share_copy(w).start()

    def communicate(n):
        reduce(n - 2 - LAG * distance)

        @pl.when((n >= EARLY) & (lax.rem(n - EARLY, RATE) == 0))
        def _():
            gather(lax.div(n - EARLY, RATE))

    @pl.loop(0, 2 * STEPS)
    def _(t):
        q = t + STEPS
        slot = lax.rem(q, 2)

        @pl.when(t == STEPS)
        def _():
            next_layer()

        wait_tile(q)

        @pl.when(q < 3 * STEPS - 1)
        def _():
            load(q + 1)

        for r in range(0, T, ROWS):
            gu = dot(A[r : r + ROWS, :], WGU[slot])
            da = dot_t(DY[r : r + ROWS, :], WD[slot]).astype(BF16).astype(F32)
            g, u = gu[:, :TILE], gu[:, TILE:]
            sig = 0.5 * jnp.tanh(0.5 * g) + 0.5
            s = g * sig
            ACT[r : r + ROWS, :] = (s * u).astype(BF16)
            DT[r : r + ROWS, TILE:] = (da * s).astype(BF16)
            DT[r : r + ROWS, :TILE] = (da * u * (sig + s * (1.0 - sig))).astype(BF16)

        communicate(2 * t)

        keep = lax.rem(t, KEEP // 2) * 2
        dgu = dot(AT[...], DT[...]).astype(BF16)
        for k in range(2):
            for half in range(2):
                OWN[keep + half, k] = dgu[:, k * TILE + half * LANES : k * TILE + (half + 1) * LANES]
        dd = dot(DYT[...], ACT[...]).astype(BF16)
        for half in range(2):
            OWN[keep + half, 2] = dd[:, half * LANES : (half + 1) * LANES]

        for half in range(2):
            v = 2 * t + half

            @pl.when(exists(v - 2))
            def _():
                part_copy(v - 2).wait_send()

            @pl.when(exists(v))
            def _():
                part_copy(v).start()

        @pl.when(t == 0)
        def _():
            ACC[...] = jnp.zeros_like(ACC)

        @pl.when(t < STEPS)
        def _():
            for r in range(0, T, ROWS):
                ACC[r : r + ROWS, :] += dot_t(DT[r : r + ROWS, :], WGU[slot])

        communicate(2 * t + 1)

    part_copy(jnp.int32(4 * STEPS - 2)).wait_send()

    @pl.loop(4 * STEPS, LAST)
    def _(n):
        communicate(n)

    for w in range(UNITS - SLOTS, UNITS):
        keep_copy(jnp.int32(w)).wait()

    def ss_copy(other):
        return pltpu.make_async_remote_copy(
            src_ref=SQ,
            dst_ref=SS.at[core],
            send_sem=sem_sssend.at[other],
            recv_sem=sem_ss.at[core],
            device_id=(rep, lax.rem(dp + other, 8)),
            device_id_type=MESH,
        )

    @pl.when(distance == 3)
    def _():
        for other in range(1, 8):
            ss_copy(other).start()
        SS[core] = SQ[...]

    @pl.loop((LAST - EARLY + RATE - 1) // RATE, UNITS + 3)
    def _(n):
        gather(n)

    everything = g_hbm.at[:, :, mine, :]
    others = g_hbm.at[:, :, theirs, :]

    @pl.when(distance > 0)
    def _():
        pltpu.make_async_copy(everything, everything, sem_gsend.at[0]).wait()

    pltpu.make_async_copy(everything, everything, sem_gd2d.at[0]).wait()
    pltpu.make_async_copy(others, others, sem_gpart.at[0]).wait()

    for piece in range(2):

        @pl.when(jnp.logical_not((distance == 3) & (core == piece)))
        def _():
            pltpu.make_async_copy(SS.at[piece], SS.at[piece], sem_ss.at[piece]).wait()

    @pl.when(distance == 3)
    def _():
        for other in range(1, 8):
            ss_copy(other).wait_send()

    ss_out[...] = SS[0] + SS[1]


def gradients(x, dy, w_gate, w_up, w_down):
    hbm = pl.BlockSpec(memory_space=pl.ANY)

    def vmem(*shape):
        return pltpu.VMEM(shape, BF16)

    dma = pltpu.SemaphoreType.DMA
    return pl.pallas_call(
        gradient_kernel,
        out_shape=(
            jax.ShapeDtypeStruct((UNITS, 3, D, LANES), BF16),
            jax.ShapeDtypeStruct((8, LANES), F32),
        ),
        in_specs=[hbm] * 5,
        out_specs=(hbm, pl.BlockSpec(memory_space=pltpu.VMEM)),
        scratch_shapes=[
            vmem(T, D), vmem(T, D), vmem(D, T), vmem(T, D), vmem(T, D), vmem(D, T),
            pltpu.VMEM((T, D), F32),
            vmem(T, 2 * TILE), vmem(T, TILE), vmem(2, D, 2 * TILE), vmem(2, TILE, D),
            vmem(KEEP, 3, D, LANES), vmem(UNITS, 3, HALF, LANES), vmem(UNITS, 3, HALF, LANES), vmem(SLOTS, 3, HALF, LANES),
            pltpu.VMEM((8, LANES), F32), pltpu.VMEM((2, 8, LANES), F32),
            dma((2,)), dma((2, 3)), dma((4,)), dma((UNITS,)), dma((UNITS,)), dma((SLOTS,)),
            dma((UNITS,)), dma((1,)), dma((1,)), dma((1,)), dma((2,)), dma((8,)),
        ],
        compiler_params=pltpu.CompilerParams(collective_id=0, has_side_effects=True, vmem_limit_bytes=63 * 2**20),
        name="gradients",
    )(x, dy, w_gate, w_up, w_down)


def update(w, m, v, g):
    m = 0.9 * m + 0.1 * g
    v = 0.95 * v + 0.05 * g * g
    step = m * lax.rsqrt(v + 1e-8) + 0.1 * w
    return (w - 0.02 * step).astype(BF16), m, v


def clip_factor(ss_ref):
    total = jnp.sum(ss_ref[...], keepdims=True)
    return jnp.minimum(1.0, 0.5 * lax.rsqrt(total / (UNITS * 3 * D * LANES) + 1e-30))


def adamw_kernel(ss, g, *refs):
    w_in, m_in, v_in, w_new, m_new, v_new = (refs[i : i + 3] for i in range(0, 18, 3))
    WI, MI, VI, GI, WO, DWI, DMI, DVI, DWO, sem_in, sem_out = refs[18:]
    factor = clip_factor(ss)

    def place(k, u):
        columns = pl.ds(pl.multiple_of(lax.rem(u, PER_LAYER) * LANES, LANES), LANES)
        layer = jnp.where(u < PER_LAYER, 1, 0)
        return (layer, slice(None), columns) if k < 2 else (layer, columns, slice(None))

    def buffers(k, u):
        slot = lax.rem(u, DEEP)
        if k < 2:
            return tuple(ref.at[slot, k] for ref in (WI, MI, VI, WO))
        return tuple(ref.at[slot] for ref in (DWI, DMI, DVI, DWO))

    def reads(k, u):
        slot, at, (w, m, v, _) = lax.rem(u, DEEP), place(k, u), buffers(k, u)
        pairs = ((w_in[k].at[at], w), (m_in[k].at[at], m), (v_in[k].at[at], v), (g.at[u, k], GI.at[slot, k]))
        return [pltpu.make_async_copy(src, dst, sem_in.at[slot, k, i]) for i, (src, dst) in enumerate(pairs)]

    def writes(k, u):
        slot, at, (_, m, v, w) = lax.rem(u, DEEP), place(k, u), buffers(k, u)
        pairs = ((w, w_new[k].at[at]), (m, m_new[k].at[at]), (v, v_new[k].at[at]))
        return [pltpu.make_async_copy(src, dst, sem_out.at[slot, k, i]) for i, (src, dst) in enumerate(pairs)]

    def start_reads(u):
        for k in range(3):
            for copy in reads(k, u):
                copy.start()

    for u in range(AHEAD):
        start_reads(jnp.int32(u))

    @pl.loop(0, UNITS)
    def _(u):
        slot = lax.rem(u, DEEP)
        later = u + AHEAD

        @pl.when(later < UNITS)
        def _():
            @pl.when(later >= DEEP)
            def _():
                for k in range(3):
                    for copy in writes(k, later - DEEP):
                        copy.wait()

            start_reads(later)

        for k in range(3):
            for copy in reads(k, u):
                copy.wait()
            w, m, v, out = buffers(k, u)
            step = 160 if k < 2 else LANES
            for r in range(0, D, step):
                piece = slice(r, r + step)
                gradient = GI[slot, k, piece, :]
                at = (piece, slice(None)) if k < 2 else (slice(None), piece)
                gradient = (gradient if k < 2 else gradient.T).astype(F32) * factor
                out[at], m[at], v[at] = update(w[at].astype(F32), m[at], v[at], gradient)
            for copy in writes(k, u):
                copy.start()

    for u in range(UNITS - DEEP, UNITS):
        for k in range(3):
            for copy in writes(k, jnp.int32(u)):
                copy.wait()


def adamw(ss, g, weights, m, v):
    hbm = pl.BlockSpec(memory_space=pl.ANY)
    dma = pltpu.SemaphoreType.DMA
    return pl.pallas_call(
        adamw_kernel,
        in_specs=[pl.BlockSpec(memory_space=pltpu.VMEM)] + [hbm] * 10,
        out_specs=(hbm,) * 9,
        out_shape=tuple(jax.ShapeDtypeStruct(a.shape, a.dtype) for a in (*weights, *m, *v)),
        scratch_shapes=[
            pltpu.VMEM((DEEP, 2, D, LANES), BF16), pltpu.VMEM((DEEP, 2, D, LANES), F32), pltpu.VMEM((DEEP, 2, D, LANES), F32),
            pltpu.VMEM((DEEP, 3, D, LANES), BF16), pltpu.VMEM((DEEP, 2, D, LANES), BF16),
            pltpu.VMEM((DEEP, LANES, D), BF16), pltpu.VMEM((DEEP, LANES, D), F32), pltpu.VMEM((DEEP, LANES, D), F32),
            pltpu.VMEM((DEEP, LANES, D), BF16), dma((DEEP, 3, 4)), dma((DEEP, 3, 3)),
        ],
        compiler_params=pltpu.CompilerParams(vmem_limit_bytes=60 * 2**20),
        name="adamw",
    )(ss, g, *weights, *m, *v)


def solution(mesh):
    def step(x, dy, *arrays):
        weights, m, v = (arrays[i : i + 3] for i in (0, 3, 6))
        g, ss = gradients(x, dy, *weights)
        return adamw(ss, g, weights, m, v)

    return jax.shard_map(
        step,
        mesh=mesh,
        in_specs=(P(("rep", "dp"), None, None),) * 2 + (P(None, None, None),) * 9,
        out_specs=(P("rep", None, None),) * 9,
        check_vma=False,
    )
```

```python
import functools

import jax
import jax.numpy as jnp
from jax import lax
from jax.experimental import pallas as pl
from jax.experimental.pallas import tpu as pltpu
from jax.sharding import PartitionSpec as P

F32, BF16 = jnp.float32, jnp.bfloat16
MESH = pl.DeviceIdType.MESH
T, D, FF = 2048, 640, 2432
TILE = 256
STEPS = 10
LANES = 128
PER_LAYER = FF // LANES
UNITS = 2 * PER_LAYER
ROWS, FORWARD_ROWS = 512, 1024
HALF = D // 2
KEEP = 10
SLOTS = 4
FIRST = 1
LAG = 2
BACK = 2
SUMMED = 2 * 2 * STEPS + FIRST + 3 * LAG
LAST = SUMMED + 3 * BACK

DEEP, AHEAD = 6, 3


def dot(a, b):
    return jnp.dot(a, b, preferred_element_type=F32)


def dot_t(a, b):
    return lax.dot_general(a, b, (((1,), (1,)), ((), ())), preferred_element_type=F32)


def norm_scale(h):
    wide = h.astype(F32)
    return wide, lax.rsqrt(jnp.mean(wide * wide, -1, keepdims=True) + 1e-6)


def gradient_kernel(
    x_hbm, dy_hbm, wg_hbm, wu_hbm, wd_hbm, G, ss_out,
    X, A, AT, H, DY, DYT, ACC, DT, ACT, WGU, WD, OWN, PART, OUT, SQ, SS,
    sem_in, sem_w, sem_d2d, sem_part, sem_up, sem_out, sem_g, sem_gsend, sem_share, sem_shared, sem_ss, sem_sssend,
):
    rep, dp = lax.axis_index("rep"), lax.axis_index("dp")
    z, core = lax.div(dp, 2), lax.rem(dp, 2)

    def at(z, core):
        return (rep, z * 2 + core)

    partner = at(z, 1 - core)
    barrier = pltpu.get_barrier_semaphore()
    for other in range(1, 8):
        pl.semaphore_signal(barrier, inc=1, device_id=(rep, lax.rem(dp + other, 8)), device_id_type=MESH)

    block = 256

    def rows_of(r):
        return pl.ds(pl.multiple_of(r * block, block), block)

    def x_copy(r):
        return pltpu.make_async_copy(x_hbm.at[0, rows_of(r), :], X.at[rows_of(r), :], sem_in.at[r])

    dy_copy = pltpu.make_async_copy(dy_hbm.at[0], DY, sem_in.at[T // block])
    for r in range(T // block):
        x_copy(jnp.int32(r)).start()

    def tile_copies(q, n):
        layer = jnp.where((q >= STEPS) & (q < 2 * STEPS), 1, 0)
        slot = lax.rem(q, 2)
        columns = pl.ds(pl.multiple_of(lax.rem(q, STEPS) * TILE, LANES), n)
        return (
            pltpu.make_async_copy(wg_hbm.at[layer, :, columns], WGU.at[slot, :, pl.ds(0, n)], sem_w.at[slot, 0]),
            pltpu.make_async_copy(wu_hbm.at[layer, :, columns], WGU.at[slot, :, pl.ds(TILE, n)], sem_w.at[slot, 1]),
            pltpu.make_async_copy(wd_hbm.at[layer, columns, :], WD.at[slot, pl.ds(0, n), :], sem_w.at[slot, 2]),
        )

    def load(q):
        short = lax.rem(q, STEPS) == STEPS - 1
        slot = lax.rem(q, 2)

        @pl.when(jnp.logical_not(short))
        def _():
            for copy in tile_copies(q, TILE):
                copy.start()

        @pl.when(short)
        def _():
            WGU[slot, :, LANES:TILE] = jnp.zeros((D, LANES), BF16)
            WGU[slot, :, TILE + LANES :] = jnp.zeros((D, LANES), BF16)
            WD[slot, LANES:, :] = jnp.zeros((LANES, D), BF16)
            for copy in tile_copies(q, LANES):
                copy.start()

    def wait_tile(q):
        short = lax.rem(q, STEPS) == STEPS - 1

        @pl.when(jnp.logical_not(short))
        def _():
            for copy in tile_copies(q, TILE):
                copy.wait()

        @pl.when(short)
        def _():
            for copy in tile_copies(q, LANES):
                copy.wait()

    load(jnp.int32(0))
    dy_copy.start()

    @pl.loop(0, T // block)
    def _(r):
        x_copy(r).wait()
        rows = rows_of(r)
        wide, scale = norm_scale(X[rows, :])
        A[rows, :] = (wide * scale).astype(BF16)

    def forward(q, first):
        slot = lax.rem(q, 2)
        wait_tile(q)
        load(q + 1)
        for r in range(0, T, FORWARD_ROWS):
            gu = dot(A[r : r + FORWARD_ROWS, :], WGU[slot])
            g, u = gu[:, :TILE], gu[:, TILE:]
            sig = 0.5 * jnp.tanh(0.5 * g) + 0.5
            h = dot((g * sig * u).astype(BF16), WD[slot])
            if first:
                ACC[r : r + FORWARD_ROWS, :] = h
            else:
                ACC[r : r + FORWARD_ROWS, :] += h
        if not first:
            rows = rows_of(jnp.minimum(q - 1, T // block - 1))
            DYT[:, rows] = DY[rows, :].T

    forward(jnp.int32(0), True)
    dy_copy.wait()

    @pl.loop(1, STEPS)
    def _(q):
        forward(q, False)

    @pl.loop(0, T // block)
    def _(r):
        rows = rows_of(r)
        h = (X[rows, :].astype(F32) + ACC[rows, :].astype(BF16).astype(F32)).astype(BF16)
        H[rows, :] = h
        wide, scale = norm_scale(h)
        a = (wide * scale).astype(BF16)
        A[rows, :] = a
        AT[:, rows] = a.T

    pl.semaphore_wait(barrier, 7)

    def next_layer():
        @pl.loop(0, T // block)
        def _(r):
            rows = rows_of(r)
            h, scale = norm_scale(H[rows, :])
            da = ACC[rows, :].astype(BF16).astype(F32)
            along = jnp.mean(da * h, -1, keepdims=True) * scale * scale
            dh = (scale * (da - h * along)).astype(BF16)
            d = (DY[rows, :].astype(F32) + dh.astype(F32)).astype(BF16)
            DY[rows, :] = d
            DYT[:, rows] = d.T
            wide, scale = norm_scale(X[rows, :])
            a = (wide * scale).astype(BF16)
            A[rows, :] = a
            AT[:, rows] = a.T

    SQ[...] = jnp.zeros_like(SQ)
    distance = jnp.where(core == 0, 3 - z, z)
    onward = jnp.where(core == 0, jnp.maximum(z - 1, 0), jnp.minimum(z + 1, 3))
    back = jnp.where(core == 0, jnp.minimum(z + 1, 3), jnp.maximum(z - 1, 0))
    mine = pl.ds(pl.multiple_of(core * HALF, 16), HALF)
    theirs = pl.ds(pl.multiple_of((1 - core) * HALF, 16), HALF)

    def exists(v):
        return (v >= 0) & (v < 4 * STEPS) & (lax.rem(v, 2 * STEPS) != 2 * STEPS - 1)

    def packed(v):
        return v - jnp.where(v >= 2 * STEPS, 1, 0)

    def part_copy(v):
        w = packed(v)
        return pltpu.make_async_remote_copy(
            src_ref=OWN.at[lax.rem(v, KEEP), :, theirs, :],
            dst_ref=PART.at[w],
            send_sem=sem_d2d.at[lax.rem(v, 4)],
            recv_sem=sem_part.at[w],
            device_id=partner,
            device_id_type=MESH,
        )

    def up_copy(w):
        return pltpu.make_async_remote_copy(
            src_ref=OUT.at[lax.rem(w, SLOTS)],
            dst_ref=G.at[w, :, mine, :],
            send_sem=sem_out.at[lax.rem(w, SLOTS)],
            recv_sem=sem_up.at[w],
            device_id=at(onward, core),
            device_id_type=MESH,
        )

    def back_copy(w):
        return pltpu.make_async_remote_copy(
            src_ref=G.at[w, :, mine, :],
            dst_ref=G.at[w, :, mine, :],
            send_sem=sem_gsend.at[0],
            recv_sem=sem_g.at[w],
            device_id=at(back, core),
            device_id_type=MESH,
        )

    def share_copy(w):
        return pltpu.make_async_remote_copy(
            src_ref=G.at[w, :, mine, :],
            dst_ref=G.at[w, :, mine, :],
            send_sem=sem_share.at[0],
            recv_sem=sem_shared.at[0],
            device_id=partner,
            device_id_type=MESH,
        )

    def reduce(v):
        @pl.when(exists(v))
        def _():
            w = packed(v)
            slot = lax.rem(w, SLOTS)
            part_copy(v).wait_recv()

            def two(k):
                return OWN[lax.rem(v, KEEP), k, mine, :].astype(F32) + PART[w, k].astype(F32)

            @pl.when((w >= SLOTS) & (distance < 3))
            def _():
                up_copy(w).wait_send()

            @pl.when(distance == 0)
            def _():
                for k in range(3):
                    OUT[slot, k] = two(k).astype(BF16)

            @pl.when(distance > 0)
            def _():
                up_copy(w).wait_recv()

            @pl.when((distance > 0) & (distance < 3))
            def _():
                for k in range(3):
                    OUT[slot, k] = (two(k) + G[w, k, mine, :].astype(F32)).astype(BF16)

            @pl.when(distance < 3)
            def _():
                up_copy(w).start()

            @pl.when(distance == 3)
            def _():
                total = jnp.zeros((8, LANES), F32)
                for k in range(3):
                    g = (two(k) + G[w, k, mine, :].astype(F32)).astype(BF16)
                    G[w, k, mine, :] = g
                    g = g.astype(F32)
                    total += jnp.sum((g * g).reshape(HALF // 8, 8, LANES), 0)
                SQ[...] += total
                back_copy(w).start()
                share_copy(w).start()

    def gather(v):
        @pl.when(exists(v) & (distance < 3))
        def _():
            w = packed(v)
            back_copy(w).wait_recv()

            @pl.when(distance > 0)
            def _():
                back_copy(w).start()

            share_copy(w).start()

    def ss_copy(other):
        return pltpu.make_async_remote_copy(
            src_ref=SQ,
            dst_ref=SS.at[core],
            send_sem=sem_sssend.at[other],
            recv_sem=sem_ss.at[core],
            device_id=(rep, lax.rem(dp + other, 8)),
            device_id_type=MESH,
        )

    def communicate(n):
        reduce(n - FIRST - LAG * distance)
        gather(n - FIRST - LAG * 3 - BACK * (3 - distance))

    @pl.loop(0, 2 * STEPS)
    def _(t):
        q = t + STEPS
        slot = lax.rem(q, 2)

        @pl.when(t == STEPS)
        def _():
            next_layer()

        wait_tile(q)

        @pl.when(q < 3 * STEPS - 1)
        def _():
            load(q + 1)

        for r in range(0, T, ROWS):
            gu = dot(A[r : r + ROWS, :], WGU[slot])
            da = dot_t(DY[r : r + ROWS, :], WD[slot]).astype(BF16).astype(F32)
            g, u = gu[:, :TILE], gu[:, TILE:]
            sig = 0.5 * jnp.tanh(0.5 * g) + 0.5
            s = g * sig
            ACT[r : r + ROWS, :] = (s * u).astype(BF16)
            DT[r : r + ROWS, TILE:] = (da * s).astype(BF16)
            DT[r : r + ROWS, :TILE] = (da * u * (sig + s * (1.0 - sig))).astype(BF16)

        communicate(2 * t)

        keep = lax.rem(t, KEEP // 2) * 2
        dgu = dot(AT[...], DT[...]).astype(BF16)
        for k in range(2):
            for half in range(2):
                OWN[keep + half, k] = dgu[:, k * TILE + half * LANES : k * TILE + (half + 1) * LANES]
        dd = dot(DYT[...], ACT[...]).astype(BF16)
        for half in range(2):
            OWN[keep + half, 2] = dd[:, half * LANES : (half + 1) * LANES]

        for half in range(2):
            v = 2 * t + half

            @pl.when(exists(v - 2))
            def _():
                part_copy(v - 2).wait_send()

            @pl.when(exists(v))
            def _():
                part_copy(v).start()

        @pl.when(t == 0)
        def _():
            ACC[...] = jnp.zeros_like(ACC)

        @pl.when(t < STEPS)
        def _():
            for r in range(0, T, ROWS):
                ACC[r : r + ROWS, :] += dot_t(DT[r : r + ROWS, :], WGU[slot])

        communicate(2 * t + 1)

    part_copy(jnp.int32(4 * STEPS - 2)).wait_send()

    @pl.loop(4 * STEPS, LAST)
    def _(n):
        communicate(n)

        @pl.when((n == SUMMED) & (distance == 3))
        def _():
            for other in range(1, 8):
                ss_copy(other).start()
            SS[core] = SQ[...]

    @pl.when(distance < 3)
    def _():
        for w in range(UNITS - SLOTS, UNITS):
            up_copy(jnp.int32(w)).wait_send()

    everything = G.at[:, :, mine, :]
    others = G.at[:, :, theirs, :]

    @pl.when(distance > 0)
    def _():
        pltpu.make_async_copy(everything, everything, sem_gsend.at[0]).wait()

    pltpu.make_async_copy(everything, everything, sem_share.at[0]).wait()
    pltpu.make_async_copy(others, others, sem_shared.at[0]).wait()

    for piece in range(2):

        @pl.when(jnp.logical_not((distance == 3) & (core == piece)))
        def _():
            pltpu.make_async_copy(SS.at[piece], SS.at[piece], sem_ss.at[piece]).wait()

    @pl.when(distance == 3)
    def _():
        for other in range(1, 8):
            ss_copy(other).wait_send()

    ss_out[...] = SS[0] + SS[1]


def gradients(x, dy, w_gate, w_up, w_down):
    hbm = pl.BlockSpec(memory_space=pl.ANY)

    def vmem(*shape):
        return pltpu.VMEM(shape, BF16)

    dma = pltpu.SemaphoreType.DMA
    return pl.pallas_call(
        gradient_kernel,
        out_shape=(vmem(UNITS, 3, D, LANES), pltpu.VMEM((8, LANES), F32)),
        in_specs=[hbm] * 5,
        out_specs=(pl.BlockSpec(memory_space=pltpu.VMEM),) * 2,
        scratch_shapes=[
            vmem(T, D), vmem(T, D), vmem(D, T), vmem(T, D), vmem(T, D), vmem(D, T),
            pltpu.VMEM((T, D), F32),
            vmem(T, 2 * TILE), vmem(T, TILE), vmem(2, D, 2 * TILE), vmem(2, TILE, D),
            vmem(KEEP, 3, D, LANES), vmem(UNITS, 3, HALF, LANES), vmem(SLOTS, 3, HALF, LANES),
            pltpu.VMEM((8, LANES), F32), pltpu.VMEM((2, 8, LANES), F32),
            dma((T // 256 + 1,)), dma((2, 3)), dma((4,)), dma((UNITS,)), dma((UNITS,)), dma((SLOTS,)),
            dma((UNITS,)), dma((1,)), dma((1,)), dma((1,)), dma((2,)), dma((8,)),
        ],
        compiler_params=pltpu.CompilerParams(collective_id=0, has_side_effects=True, vmem_limit_bytes=46 * 2**20),
        name="gradients",
    )(x, dy, w_gate, w_up, w_down)


def update(w, m, v, g):
    m = 0.9 * m + 0.1 * g
    v = 0.95 * v + 0.05 * g * g
    step = m * lax.rsqrt(v + 1e-8) + 0.1 * w
    return (w - 0.02 * step).astype(BF16), m, v


def clip_factor(ss_ref):
    total = jnp.sum(ss_ref[...], keepdims=True)
    return jnp.minimum(1.0, 0.5 * lax.rsqrt(total / (UNITS * 3 * D * LANES) + 1e-30))


def adamw_kernel(ss, g, *refs):
    w_in, m_in, v_in, w_new, m_new, v_new = (refs[i : i + 3] for i in range(0, 18, 3))
    WI, MI, VI, WO, DWI, DMI, DVI, DWO, sem_in, sem_out = refs[18:]
    factor = clip_factor(ss)

    def place(k, u):
        columns = pl.ds(pl.multiple_of(lax.rem(u, PER_LAYER) * LANES, LANES), LANES)
        layer = jnp.where(u < PER_LAYER, 1, 0)
        return (layer, slice(None), columns) if k < 2 else (layer, columns, slice(None))

    def buffers(k, u):
        slot = lax.rem(u, DEEP)
        if k < 2:
            return tuple(ref.at[slot, k] for ref in (WI, MI, VI, WO))
        return tuple(ref.at[slot] for ref in (DWI, DMI, DVI, DWO))

    def reads(k, u):
        slot, at, (w, m, v, _) = lax.rem(u, DEEP), place(k, u), buffers(k, u)
        pairs = ((w_in[k].at[at], w), (m_in[k].at[at], m), (v_in[k].at[at], v))
        return [pltpu.make_async_copy(src, dst, sem_in.at[slot, k, i]) for i, (src, dst) in enumerate(pairs)]

    def writes(k, u):
        slot, at, (_, m, v, w) = lax.rem(u, DEEP), place(k, u), buffers(k, u)
        pairs = ((w, w_new[k].at[at]), (m, m_new[k].at[at]), (v, v_new[k].at[at]))
        return [pltpu.make_async_copy(src, dst, sem_out.at[slot, k, i]) for i, (src, dst) in enumerate(pairs)]

    def start_reads(u):
        for k in range(3):
            for copy in reads(k, u):
                copy.start()

    for u in range(AHEAD):
        start_reads(jnp.int32(u))

    @pl.loop(0, UNITS)
    def _(u):
        later = u + AHEAD

        @pl.when(later < UNITS)
        def _():
            @pl.when(later >= DEEP)
            def _():
                for k in range(3):
                    for copy in writes(k, later - DEEP):
                        copy.wait()

            start_reads(later)

        for k in range(3):
            for copy in reads(k, u):
                copy.wait()
            w, m, v, out = buffers(k, u)
            step = 160 if k < 2 else LANES
            for r in range(0, D, step):
                piece = slice(r, r + step)
                gradient = g[u, k, piece, :]
                at = (piece, slice(None)) if k < 2 else (slice(None), piece)
                gradient = (gradient if k < 2 else gradient.T).astype(F32) * factor
                out[at], m[at], v[at] = update(w[at].astype(F32), m[at], v[at], gradient)
            for copy in writes(k, u):
                copy.start()

    for u in range(UNITS - DEEP, UNITS):
        for k in range(3):
            for copy in writes(k, jnp.int32(u)):
                copy.wait()


def adamw(ss, g, weights, m, v):
    hbm = pl.BlockSpec(memory_space=pltpu.HBM)
    ss, g = (pltpu.with_memory_space_constraint(a, pltpu.VMEM) for a in (ss, g))
    dma = pltpu.SemaphoreType.DMA
    return pl.pallas_call(
        adamw_kernel,
        in_specs=[pl.BlockSpec(memory_space=pltpu.VMEM)] * 2 + [hbm] * 9,
        out_specs=(hbm,) * 9,
        out_shape=tuple(jax.ShapeDtypeStruct(a.shape, a.dtype) for a in (*weights, *m, *v)),
        scratch_shapes=[
            pltpu.VMEM((DEEP, 2, D, LANES), BF16), pltpu.VMEM((DEEP, 2, D, LANES), F32), pltpu.VMEM((DEEP, 2, D, LANES), F32),
            pltpu.VMEM((DEEP, 2, D, LANES), BF16),
            pltpu.VMEM((DEEP, LANES, D), BF16), pltpu.VMEM((DEEP, LANES, D), F32), pltpu.VMEM((DEEP, LANES, D), F32),
            pltpu.VMEM((DEEP, LANES, D), BF16), dma((DEEP, 3, 3)), dma((DEEP, 3, 3)),
        ],
        compiler_params=pltpu.CompilerParams(vmem_limit_bytes=46 * 2**20),
        name="adamw",
    )(ss, g, *weights, *m, *v)


def solution(mesh):
    def step(x, dy, *arrays):
        weights, m, v = (arrays[i : i + 3] for i in (0, 3, 6))
        g, ss = gradients(x, dy, *weights)
        return adamw(ss, g, weights, m, v)

    return jax.shard_map(
        step,
        mesh=mesh,
        in_specs=(P(("rep", "dp"), None, None),) * 2 + (P(None, None, None),) * 9,
        out_specs=(P("rep", None, None),) * 9,
        check_vma=False,
    )
```

```python
import functools

import jax
import jax.numpy as jnp
from jax import lax
from jax.experimental import pallas as pl
from jax.experimental.pallas import tpu as pltpu
from jax.sharding import PartitionSpec as P

F32, BF16 = jnp.float32, jnp.bfloat16
MESH = pl.DeviceIdType.MESH
T, D, FF = 2048, 640, 2432
TILE = 256
STEPS = 10
LANES = 128
PER_LAYER = FF // LANES
UNITS = 2 * PER_LAYER
ROWS, FORWARD_ROWS = 512, 1024
HALF = D // 2
KEEP = 10
SLOTS = 4
FIRST = 1
LAG = 2
BACK = 2
SUMMED = 2 * 2 * STEPS + FIRST + 3 * LAG
LAST = SUMMED + 3 * BACK
AT_A_TIME = -(-UNITS // (LAST - SUMMED))

DEEP, AHEAD = 6, 3
AHEAD_UNITS = T // LANES


def dot(a, b):
    return jnp.dot(a, b, preferred_element_type=F32)


def dot_t(a, b):
    return lax.dot_general(a, b, (((1,), (1,)), ((), ())), preferred_element_type=F32)


def norm_scale(h):
    wide = h.astype(F32)
    return wide, lax.rsqrt(jnp.mean(wide * wide, -1, keepdims=True) + 1e-6)


def gradient_kernel(
    x_hbm, dy_hbm, wg_hbm, wu_hbm, wd_hbm, md_hbm, G, ss_out, XA, ATS, PART, ACC,
    H, DY, DT, ACT, WGU, WD, OWN, OUT, SQ, SS, sem_ahead,
    sem_in, sem_w, sem_d2d, sem_part, sem_up, sem_out, sem_g, sem_gsend, sem_share, sem_shared, sem_ss, sem_sssend,
):
    X, A, AT, DYT = XA.at[0], XA.at[1], ATS.at[0], ATS.at[1]
    rep, dp = lax.axis_index("rep"), lax.axis_index("dp")
    z, core = lax.div(dp, 2), lax.rem(dp, 2)

    def at(z, core):
        return (rep, z * 2 + core)

    partner = at(z, 1 - core)
    barrier = pltpu.get_barrier_semaphore()
    for other in range(1, 8):
        pl.semaphore_signal(barrier, inc=1, device_id=(rep, lax.rem(dp + other, 8)), device_id_type=MESH)

    block = 256

    def rows_of(r):
        return pl.ds(pl.multiple_of(r * block, block), block)

    def x_copy(r):
        return pltpu.make_async_copy(x_hbm.at[0, rows_of(r), :], X.at[rows_of(r), :], sem_in.at[r])

    dy_copy = pltpu.make_async_copy(dy_hbm.at[0], DY, sem_in.at[T // block])
    for r in range(T // block):
        x_copy(jnp.int32(r)).start()

    def tile_copies(q, n):
        layer = jnp.where((q >= STEPS) & (q < 2 * STEPS), 1, 0)
        slot = lax.rem(q, 2)
        columns = pl.ds(pl.multiple_of(lax.rem(q, STEPS) * TILE, LANES), n)
        return (
            pltpu.make_async_copy(wg_hbm.at[layer, :, columns], WGU.at[slot, :, pl.ds(0, n)], sem_w.at[slot, 0]),
            pltpu.make_async_copy(wu_hbm.at[layer, :, columns], WGU.at[slot, :, pl.ds(TILE, n)], sem_w.at[slot, 1]),
            pltpu.make_async_copy(wd_hbm.at[layer, columns, :], WD.at[slot, pl.ds(0, n), :], sem_w.at[slot, 2]),
        )

    def load(q):
        short = lax.rem(q, STEPS) == STEPS - 1
        slot = lax.rem(q, 2)

        @pl.when(jnp.logical_not(short))
        def _():
            for copy in tile_copies(q, TILE):
                copy.start()

        @pl.when(short)
        def _():
            WGU[slot, :, LANES:TILE] = jnp.zeros((D, LANES), BF16)
            WGU[slot, :, TILE + LANES :] = jnp.zeros((D, LANES), BF16)
            WD[slot, LANES:, :] = jnp.zeros((LANES, D), BF16)
            for copy in tile_copies(q, LANES):
                copy.start()

    def wait_tile(q):
        short = lax.rem(q, STEPS) == STEPS - 1

        @pl.when(jnp.logical_not(short))
        def _():
            for copy in tile_copies(q, TILE):
                copy.wait()

        @pl.when(short)
        def _():
            for copy in tile_copies(q, LANES):
                copy.wait()

    load(jnp.int32(0))
    dy_copy.start()

    @pl.loop(0, T // block)
    def _(r):
        x_copy(r).wait()
        rows = rows_of(r)
        wide, scale = norm_scale(X[rows, :])
        A[rows, :] = (wide * scale).astype(BF16)

    def forward(q, first):
        slot = lax.rem(q, 2)
        wait_tile(q)
        load(q + 1)
        for r in range(0, T, FORWARD_ROWS):
            gu = dot(A[r : r + FORWARD_ROWS, :], WGU[slot])
            g, u = gu[:, :TILE], gu[:, TILE:]
            sig = 0.5 * jnp.tanh(0.5 * g) + 0.5
            h = dot((g * sig * u).astype(BF16), WD[slot])
            if first:
                ACC[r : r + FORWARD_ROWS, :] = h
            else:
                ACC[r : r + FORWARD_ROWS, :] += h
        if not first:
            rows = rows_of(jnp.minimum(q - 1, T // block - 1))
            DYT[:, rows] = DY[rows, :].T

    forward(jnp.int32(0), True)
    dy_copy.wait()

    @pl.loop(1, STEPS)
    def _(q):
        forward(q, False)

    @pl.loop(0, T // block)
    def _(r):
        rows = rows_of(r)
        h = (X[rows, :].astype(F32) + ACC[rows, :].astype(BF16).astype(F32)).astype(BF16)
        H[rows, :] = h
        wide, scale = norm_scale(h)
        a = (wide * scale).astype(BF16)
        A[rows, :] = a
        AT[:, rows] = a.T

    pl.semaphore_wait(barrier, 7)

    def next_layer():
        @pl.loop(0, T // block)
        def _(r):
            rows = rows_of(r)
            h, scale = norm_scale(H[rows, :])
            da = ACC[rows, :].astype(BF16).astype(F32)
            along = jnp.mean(da * h, -1, keepdims=True) * scale * scale
            dh = (scale * (da - h * along)).astype(BF16)
            d = (DY[rows, :].astype(F32) + dh.astype(F32)).astype(BF16)
            DY[rows, :] = d
            DYT[:, rows] = d.T
            wide, scale = norm_scale(X[rows, :])
            a = (wide * scale).astype(BF16)
            A[rows, :] = a
            AT[:, rows] = a.T

    SQ[...] = jnp.zeros_like(SQ)
    distance = jnp.where(core == 0, 3 - z, z)
    onward = jnp.where(core == 0, jnp.maximum(z - 1, 0), jnp.minimum(z + 1, 3))
    back = jnp.where(core == 0, jnp.minimum(z + 1, 3), jnp.maximum(z - 1, 0))
    mine = pl.ds(pl.multiple_of(core * HALF, 16), HALF)
    theirs = pl.ds(pl.multiple_of((1 - core) * HALF, 16), HALF)

    def exists(v):
        return (v >= 0) & (v < 4 * STEPS) & (lax.rem(v, 2 * STEPS) != 2 * STEPS - 1)

    def packed(v):
        return v - jnp.where(v >= 2 * STEPS, 1, 0)

    def part_copy(v):
        w = packed(v)
        return pltpu.make_async_remote_copy(
            src_ref=OWN.at[lax.rem(v, KEEP), :, theirs, :],
            dst_ref=PART.at[w],
            send_sem=sem_d2d.at[lax.rem(v, 4)],
            recv_sem=sem_part.at[w],
            device_id=partner,
            device_id_type=MESH,
        )

    def up_copy(w):
        return pltpu.make_async_remote_copy(
            src_ref=OUT.at[lax.rem(w, SLOTS)],
            dst_ref=G.at[w, :, mine, :],
            send_sem=sem_out.at[lax.rem(w, SLOTS)],
            recv_sem=sem_up.at[w],
            device_id=at(onward, core),
            device_id_type=MESH,
        )

    def back_copy(w):
        return pltpu.make_async_remote_copy(
            src_ref=G.at[w, :, mine, :],
            dst_ref=G.at[w, :, mine, :],
            send_sem=sem_gsend.at[0],
            recv_sem=sem_g.at[w],
            device_id=at(back, core),
            device_id_type=MESH,
        )

    def share_copy(w):
        return pltpu.make_async_remote_copy(
            src_ref=G.at[w, :, mine, :],
            dst_ref=G.at[w, :, mine, :],
            send_sem=sem_share.at[0],
            recv_sem=sem_shared.at[0],
            device_id=partner,
            device_id_type=MESH,
        )

    def reduce(v):
        @pl.when(exists(v))
        def _():
            w = packed(v)
            slot = lax.rem(w, SLOTS)
            part_copy(v).wait_recv()

            def two(k):
                return OWN[lax.rem(v, KEEP), k, mine, :].astype(F32) + PART[w, k].astype(F32)

            @pl.when((w >= SLOTS) & (distance < 3))
            def _():
                up_copy(w).wait_send()

            @pl.when(distance == 0)
            def _():
                for k in range(3):
                    OUT[slot, k] = two(k).astype(BF16)

            @pl.when(distance > 0)
            def _():
                up_copy(w).wait_recv()

            @pl.when((distance > 0) & (distance < 3))
            def _():
                for k in range(3):
                    OUT[slot, k] = (two(k) + G[w, k, mine, :].astype(F32)).astype(BF16)

            @pl.when(distance < 3)
            def _():
                up_copy(w).start()

            @pl.when(distance == 3)
            def _():
                total = jnp.zeros((8, LANES), F32)
                for k in range(3):
                    g = (two(k) + G[w, k, mine, :].astype(F32)).astype(BF16)
                    G[w, k, mine, :] = g
                    g = g.astype(F32)
                    total += jnp.sum((g * g).reshape(HALF // 8, 8, LANES), 0)
                SQ[...] += total
                back_copy(w).start()
                share_copy(w).start()

    def gather(v):
        @pl.when(exists(v) & (distance < 3))
        def _():
            w = packed(v)
            back_copy(w).wait_recv()

            @pl.when(distance > 0)
            def _():
                back_copy(w).start()

            share_copy(w).start()

    def ss_copy(other):
        return pltpu.make_async_remote_copy(
            src_ref=SQ,
            dst_ref=SS.at[core],
            send_sem=sem_sssend.at[other],
            recv_sem=sem_ss.at[core],
            device_id=(rep, lax.rem(dp + other, 8)),
            device_id_type=MESH,
        )

    def communicate(n):
        reduce(n - FIRST - LAG * distance)
        gather(n - FIRST - LAG * 3 - BACK * (3 - distance))

    @pl.loop(0, 2 * STEPS)
    def _(t):
        q = t + STEPS
        slot = lax.rem(q, 2)

        @pl.when(t == STEPS)
        def _():
            next_layer()

        wait_tile(q)

        @pl.when(q < 3 * STEPS - 1)
        def _():
            load(q + 1)

        for r in range(0, T, ROWS):
            gu = dot(A[r : r + ROWS, :], WGU[slot])
            da = dot_t(DY[r : r + ROWS, :], WD[slot]).astype(BF16).astype(F32)
            g, u = gu[:, :TILE], gu[:, TILE:]
            sig = 0.5 * jnp.tanh(0.5 * g) + 0.5
            s = g * sig
            ACT[r : r + ROWS, :] = (s * u).astype(BF16)
            DT[r : r + ROWS, TILE:] = (da * s).astype(BF16)
            DT[r : r + ROWS, :TILE] = (da * u * (sig + s * (1.0 - sig))).astype(BF16)

        communicate(2 * t)

        keep = lax.rem(t, KEEP // 2) * 2
        dgu = dot(AT[...], DT[...]).astype(BF16)
        for k in range(2):
            for half in range(2):
                OWN[keep + half, k] = dgu[:, k * TILE + half * LANES : k * TILE + (half + 1) * LANES]
        dd = dot(DYT[...], ACT[...]).astype(BF16)
        for half in range(2):
            OWN[keep + half, 2] = dd[:, half * LANES : (half + 1) * LANES]

        for half in range(2):
            v = 2 * t + half

            @pl.when(exists(v - 2))
            def _():
                part_copy(v - 2).wait_send()

            @pl.when(exists(v))
            def _():
                part_copy(v).start()

        @pl.when(t == 0)
        def _():
            ACC[...] = jnp.zeros_like(ACC)

        @pl.when(t < STEPS)
        def _():
            for r in range(0, T, ROWS):
                ACC[r : r + ROWS, :] += dot_t(DT[r : r + ROWS, :], WGU[slot])

        communicate(2 * t + 1)

    part_copy(jnp.int32(4 * STEPS - 2)).wait_send()

    whole = pl.ds(0, AHEAD_UNITS * LANES)
    ahead = (
        pltpu.make_async_copy(wd_hbm.at[:, whole, :], XA, sem_ahead.at[0]),
        pltpu.make_async_copy(wg_hbm.at[:, :, whole], ATS, sem_ahead.at[1]),
        pltpu.make_async_copy(md_hbm.at[1, whole, :], ACC, sem_ahead.at[2]),
    )
    for copy in ahead:
        copy.start()

    def up_ahead(u, half):
        columns = pl.ds(pl.multiple_of(lax.rem(u, PER_LAYER) * LANES, LANES), LANES)
        rows = pl.ds(half * HALF, HALF)
        return pltpu.make_async_copy(wu_hbm.at[jnp.where(u < PER_LAYER, 1, 0), rows, columns], PART.at[u, half], sem_ahead.at[3])

    @pl.loop(4 * STEPS, LAST)
    def _(n):
        communicate(n)

        @pl.when(n >= SUMMED)
        def _():
            first = (n - SUMMED) * AT_A_TIME

            @pl.loop(first, jnp.minimum(first + AT_A_TIME, UNITS))
            def _(u):
                for half in range(2):
                    up_ahead(u, half).start()

        @pl.when((n == SUMMED) & (distance == 3))
        def _():
            for other in range(1, 8):
                ss_copy(other).start()
            SS[core] = SQ[...]

    @pl.when(distance < 3)
    def _():
        for w in range(UNITS - SLOTS, UNITS):
            up_copy(jnp.int32(w)).wait_send()

    everything = G.at[:, :, mine, :]
    others = G.at[:, :, theirs, :]

    @pl.when(distance > 0)
    def _():
        pltpu.make_async_copy(everything, everything, sem_gsend.at[0]).wait()

    pltpu.make_async_copy(everything, everything, sem_share.at[0]).wait()
    pltpu.make_async_copy(others, others, sem_shared.at[0]).wait()

    for copy in ahead:
        copy.wait()
    landed = PART.at[:, pl.ds(0, 2)]
    pltpu.make_async_copy(landed, landed, sem_ahead.at[3]).wait()

    for piece in range(2):

        @pl.when(jnp.logical_not((distance == 3) & (core == piece)))
        def _():
            pltpu.make_async_copy(SS.at[piece], SS.at[piece], sem_ss.at[piece]).wait()

    @pl.when(distance == 3)
    def _():
        for other in range(1, 8):
            ss_copy(other).wait_send()

    ss_out[...] = SS[0] + SS[1]


def gradients(x, dy, w_gate, w_up, w_down, m_down):
    hbm = pl.BlockSpec(memory_space=pl.ANY)

    def vmem(*shape):
        return pltpu.VMEM(shape, BF16)

    dma = pltpu.SemaphoreType.DMA
    return pl.pallas_call(
        gradient_kernel,
        out_shape=(
            vmem(UNITS, 3, D, LANES), pltpu.VMEM((8, LANES), F32),
            vmem(2, T, D), vmem(2, D, T), vmem(UNITS, 3, HALF, LANES), pltpu.VMEM((T, D), F32),
        ),
        in_specs=[hbm] * 6,
        out_specs=(pl.BlockSpec(memory_space=pltpu.VMEM),) * 6,
        scratch_shapes=[
            vmem(T, D), vmem(T, D),
            vmem(T, 2 * TILE), vmem(T, TILE), vmem(2, D, 2 * TILE), vmem(2, TILE, D),
            vmem(KEEP, 3, D, LANES), vmem(SLOTS, 3, HALF, LANES),
            pltpu.VMEM((8, LANES), F32), pltpu.VMEM((2, 8, LANES), F32), dma((4,)),
            dma((T // 256 + 1,)), dma((2, 3)), dma((4,)), dma((UNITS,)), dma((UNITS,)), dma((SLOTS,)),
            dma((UNITS,)), dma((1,)), dma((1,)), dma((1,)), dma((2,)), dma((8,)),
        ],
        compiler_params=pltpu.CompilerParams(collective_id=0, has_side_effects=True, vmem_limit_bytes=22 * 2**20),
        name="gradients",
    )(x, dy, w_gate, w_up, w_down, m_down)


def update(w, m, v, g):
    m = 0.9 * m + 0.1 * g
    v = 0.95 * v + 0.05 * g * g
    step = m * lax.rsqrt(v + 1e-8) + 0.1 * w
    return (w - 0.02 * step).astype(BF16), m, v


def clip_factor(ss_ref):
    total = jnp.sum(ss_ref[...], keepdims=True)
    return jnp.minimum(1.0, 0.5 * lax.rsqrt(total / (UNITS * 3 * D * LANES) + 1e-30))


def adamw_kernel(ss, g, w_down_ahead, w_gate_ahead, w_up_ahead, m_down_ahead, *refs):
    w_in, m_in, v_in, w_new, m_new, v_new = (refs[i : i + 3] for i in range(0, 18, 3))
    WI, MI, VI, WO, DWI, DMI, DVI, DWO, sem_in, sem_out = refs[18:]
    factor = clip_factor(ss)

    def place(k, u):
        columns = pl.ds(pl.multiple_of(lax.rem(u, PER_LAYER) * LANES, LANES), LANES)
        layer = jnp.where(u < PER_LAYER, 1, 0)
        return (layer, slice(None), columns) if k < 2 else (layer, columns, slice(None))

    def buffers(k, u):
        slot = lax.rem(u, DEEP)
        if k < 2:
            return tuple(ref.at[slot, k] for ref in (WI, MI, VI, WO))
        return tuple(ref.at[slot] for ref in (DWI, DMI, DVI, DWO))

    def reads(k, u):
        slot, at, (w, m, v, _) = lax.rem(u, DEEP), place(k, u), buffers(k, u)
        pairs = ((w_in[k].at[at], w), (m_in[k].at[at], m), (v_in[k].at[at], v))
        return [pltpu.make_async_copy(src, dst, sem_in.at[slot, k, i]) for i, (src, dst) in enumerate(pairs)]

    def is_ahead(u):
        return lax.rem(u, PER_LAYER) < AHEAD_UNITS

    def each_read(k, u, act):
        w, m, v = reads(k, u)
        act(v)
        if k == 2:
            pl.when(jnp.logical_not(is_ahead(u) & (u < PER_LAYER)))(lambda: act(m))
        else:
            act(m)
        if k != 1:
            pl.when(jnp.logical_not(is_ahead(u)))(lambda: act(w))

    def writes(k, u):
        slot, at, (_, m, v, w) = lax.rem(u, DEEP), place(k, u), buffers(k, u)
        pairs = ((w, w_new[k].at[at]), (m, m_new[k].at[at]), (v, v_new[k].at[at]))
        return [pltpu.make_async_copy(src, dst, sem_out.at[slot, k, i]) for i, (src, dst) in enumerate(pairs)]

    def start_reads(u):
        for k in range(3):
            each_read(k, u, lambda copy: copy.start())

    for u in range(AHEAD):
        start_reads(jnp.int32(u))

    @pl.loop(0, UNITS)
    def _(u):
        later = u + AHEAD

        @pl.when(later < UNITS)
        def _():
            @pl.when(later >= DEEP)
            def _():
                for k in range(3):
                    for copy in writes(k, later - DEEP):
                        copy.wait()

            start_reads(later)

        layer = jnp.where(u < PER_LAYER, 1, 0)
        columns = pl.ds(pl.multiple_of(lax.rem(u, PER_LAYER) * LANES, LANES), LANES)

        def new_values(k, old_w, old_m):
            w, m, v, out = buffers(k, u)
            step = 160 if k < 2 else LANES
            for r in range(0, D, step):
                piece = slice(r, r + step)
                gradient = g[u, k, piece, :]
                at = (piece, slice(None)) if k < 2 else (slice(None), piece)
                gradient = (gradient if k < 2 else gradient.T).astype(F32) * factor
                out[at], m[at], v[at] = update(old_w(r, at).astype(F32), old_m(at), v[at], gradient)

        def read_w(k):
            return lambda r, at: buffers(k, u)[0][at]

        def read_m(k):
            return lambda at: buffers(k, u)[1][at]

        def down_w(r, at):
            return w_down_ahead[layer, columns, at[1]]

        for k in range(3):
            each_read(k, u, lambda copy: copy.wait())
            if k == 0:
                pl.when(is_ahead(u))(lambda: new_values(0, lambda r, at: w_gate_ahead[layer, at[0], columns], read_m(0)))
                pl.when(jnp.logical_not(is_ahead(u)))(lambda: new_values(0, read_w(0), read_m(0)))
            elif k == 1:
                new_values(1, lambda r, at: w_up_ahead[u, r // HALF, r % HALF : r % HALF + 160, :], read_m(1))
            else:
                both = is_ahead(u) & (u < PER_LAYER)
                pl.when(both)(lambda: new_values(2, down_w, lambda at: m_down_ahead[columns, at[1]]))
                pl.when(is_ahead(u) & (u >= PER_LAYER))(lambda: new_values(2, down_w, read_m(2)))
                pl.when(jnp.logical_not(is_ahead(u)))(lambda: new_values(2, read_w(2), read_m(2)))
            for copy in writes(k, u):
                copy.start()

    for u in range(UNITS - DEEP, UNITS):
        for k in range(3):
            for copy in writes(k, jnp.int32(u)):
                copy.wait()


def adamw(ss, g, ahead, weights, m, v):
    hbm = pl.BlockSpec(memory_space=pltpu.HBM)
    near = [pltpu.with_memory_space_constraint(a, pltpu.VMEM) for a in (ss, g, *ahead)]
    dma = pltpu.SemaphoreType.DMA
    return pl.pallas_call(
        adamw_kernel,
        in_specs=[pl.BlockSpec(memory_space=pltpu.VMEM)] * 6 + [hbm] * 9,
        out_specs=(hbm,) * 9,
        out_shape=tuple(jax.ShapeDtypeStruct(a.shape, a.dtype) for a in (*weights, *m, *v)),
        scratch_shapes=[
            pltpu.VMEM((DEEP, 2, D, LANES), BF16), pltpu.VMEM((DEEP, 2, D, LANES), F32), pltpu.VMEM((DEEP, 2, D, LANES), F32),
            pltpu.VMEM((DEEP, 2, D, LANES), BF16),
            pltpu.VMEM((DEEP, LANES, D), BF16), pltpu.VMEM((DEEP, LANES, D), F32), pltpu.VMEM((DEEP, LANES, D), F32),
            pltpu.VMEM((DEEP, LANES, D), BF16), dma((DEEP, 3, 3)), dma((DEEP, 3, 3)),
        ],
        compiler_params=pltpu.CompilerParams(vmem_limit_bytes=22 * 2**20),
        name="adamw",
    )(*near, *weights, *m, *v)


def solution(mesh):
    def step(x, dy, *arrays):
        weights, m, v = (arrays[i : i + 3] for i in (0, 3, 6))
        g, ss, *ahead = gradients(x, dy, *weights, m[2])
        return adamw(ss, g, ahead, weights, m, v)

    return jax.shard_map(
        step,
        mesh=mesh,
        in_specs=(P(("rep", "dp"), None, None),) * 2 + (P(None, None, None),) * 9,
        out_specs=(P("rep", None, None),) * 9,
        check_vma=False,
    )
```

```python
import functools

import jax
import jax.numpy as jnp
from jax import lax
from jax.experimental import pallas as pl
from jax.experimental.pallas import tpu as pltpu
from jax.sharding import PartitionSpec as P

F32, BF16 = jnp.float32, jnp.bfloat16
MESH = pl.DeviceIdType.MESH
T, D, FF = 2048, 640, 2432
TILE = 256
STEPS = 10
LANES = 128
PER_LAYER = FF // LANES
UNITS = 2 * PER_LAYER
ROWS, FORWARD_ROWS = 512, 1024
HALF = D // 2
KEEP = 10
SLOTS = 4
FIRST = 1
LAG = 2
BACK = 2
SUMMED = 2 * 2 * STEPS + FIRST + 3 * LAG
LAST = SUMMED + 3 * BACK
AT_A_TIME = -(-UNITS // (LAST - SUMMED))

DEEP, AHEAD = 6, 4
AHEAD_UNITS = T // LANES


def dot(a, b):
    return jnp.dot(a, b, preferred_element_type=F32)


def dot_t(a, b):
    return lax.dot_general(a, b, (((1,), (1,)), ((), ())), preferred_element_type=F32)


def norm_scale(h):
    wide = h.astype(F32)
    return wide, lax.rsqrt(jnp.mean(wide * wide, -1, keepdims=True) + 1e-6)


def gradient_kernel(
    x_hbm, dy_hbm, wg_hbm, wu_hbm, wd_hbm, md_hbm, G, ss_out, XA, ATS, PART, ACC,
    H, DY, DT, ACT, WGU, WD, OWN, OUT, SQ, SS, sem_ahead,
    sem_in, sem_w, sem_d2d, sem_part, sem_up, sem_out, sem_g, sem_gsend, sem_share, sem_shared, sem_ss, sem_sssend,
):
    X, A, AT, DYT = XA.at[0], XA.at[1], ATS.at[0], ATS.at[1]
    rep, dp = lax.axis_index("rep"), lax.axis_index("dp")
    z, core = lax.div(dp, 2), lax.rem(dp, 2)

    def at(z, core):
        return (rep, z * 2 + core)

    partner = at(z, 1 - core)
    barrier = pltpu.get_barrier_semaphore()
    for other in range(1, 8):
        pl.semaphore_signal(barrier, inc=1, device_id=(rep, lax.rem(dp + other, 8)), device_id_type=MESH)

    block = 256

    def rows_of(r):
        return pl.ds(pl.multiple_of(r * block, block), block)

    def x_copy(r):
        return pltpu.make_async_copy(x_hbm.at[0, rows_of(r), :], X.at[rows_of(r), :], sem_in.at[r])

    dy_copy = pltpu.make_async_copy(dy_hbm.at[0], DY, sem_in.at[T // block])
    for r in range(T // block):
        x_copy(jnp.int32(r)).start()

    def tile_copies(q, n):
        layer = jnp.where((q >= STEPS) & (q < 2 * STEPS), 1, 0)
        slot = lax.rem(q, 2)
        columns = pl.ds(pl.multiple_of(lax.rem(q, STEPS) * TILE, LANES), n)
        return (
            pltpu.make_async_copy(wg_hbm.at[layer, :, columns], WGU.at[slot, :, pl.ds(0, n)], sem_w.at[slot, 0]),
            pltpu.make_async_copy(wu_hbm.at[layer, :, columns], WGU.at[slot, :, pl.ds(TILE, n)], sem_w.at[slot, 1]),
            pltpu.make_async_copy(wd_hbm.at[layer, columns, :], WD.at[slot, pl.ds(0, n), :], sem_w.at[slot, 2]),
        )

    def load(q):
        short = lax.rem(q, STEPS) == STEPS - 1
        slot = lax.rem(q, 2)

        @pl.when(jnp.logical_not(short))
        def _():
            for copy in tile_copies(q, TILE):
                copy.start()

        @pl.when(short)
        def _():
            WGU[slot, :, LANES:TILE] = jnp.zeros((D, LANES), BF16)
            WGU[slot, :, TILE + LANES :] = jnp.zeros((D, LANES), BF16)
            WD[slot, LANES:, :] = jnp.zeros((LANES, D), BF16)
            for copy in tile_copies(q, LANES):
                copy.start()

    def wait_tile(q):
        short = lax.rem(q, STEPS) == STEPS - 1

        @pl.when(jnp.logical_not(short))
        def _():
            for copy in tile_copies(q, TILE):
                copy.wait()

        @pl.when(short)
        def _():
            for copy in tile_copies(q, LANES):
                copy.wait()

    load(jnp.int32(0))
    dy_copy.start()

    @pl.loop(0, T // block)
    def _(r):
        x_copy(r).wait()
        rows = rows_of(r)
        wide, scale = norm_scale(X[rows, :])
        A[rows, :] = (wide * scale).astype(BF16)

    def forward(q, first):
        slot = lax.rem(q, 2)
        wait_tile(q)
        load(q + 1)
        for r in range(0, T, FORWARD_ROWS):
            gu = dot(A[r : r + FORWARD_ROWS, :], WGU[slot])
            g, u = gu[:, :TILE], gu[:, TILE:]
            sig = 0.5 * jnp.tanh(0.5 * g) + 0.5
            h = dot((g * sig * u).astype(BF16), WD[slot])
            if first:
                ACC[r : r + FORWARD_ROWS, :] = h
            else:
                ACC[r : r + FORWARD_ROWS, :] += h
        if not first:
            rows = rows_of(jnp.minimum(q - 1, T // block - 1))
            DYT[:, rows] = DY[rows, :].T

    forward(jnp.int32(0), True)
    dy_copy.wait()

    @pl.loop(1, STEPS)
    def _(q):
        forward(q, False)

    @pl.loop(0, T // block)
    def _(r):
        rows = rows_of(r)
        h = (X[rows, :].astype(F32) + ACC[rows, :].astype(BF16).astype(F32)).astype(BF16)
        H[rows, :] = h
        wide, scale = norm_scale(h)
        a = (wide * scale).astype(BF16)
        A[rows, :] = a
        AT[:, rows] = a.T

    pl.semaphore_wait(barrier, 7)

    def next_layer():
        @pl.loop(0, T // block)
        def _(r):
            rows = rows_of(r)
            h, scale = norm_scale(H[rows, :])
            da = ACC[rows, :].astype(BF16).astype(F32)
            along = jnp.mean(da * h, -1, keepdims=True) * scale * scale
            dh = (scale * (da - h * along)).astype(BF16)
            d = (DY[rows, :].astype(F32) + dh.astype(F32)).astype(BF16)
            DY[rows, :] = d
            DYT[:, rows] = d.T
            wide, scale = norm_scale(X[rows, :])
            a = (wide * scale).astype(BF16)
            A[rows, :] = a
            AT[:, rows] = a.T

    SQ[...] = jnp.zeros_like(SQ)
    distance = jnp.where(core == 0, 3 - z, z)
    onward = jnp.where(core == 0, jnp.maximum(z - 1, 0), jnp.minimum(z + 1, 3))
    back = jnp.where(core == 0, jnp.minimum(z + 1, 3), jnp.maximum(z - 1, 0))
    mine = pl.ds(pl.multiple_of(core * HALF, 16), HALF)
    theirs = pl.ds(pl.multiple_of((1 - core) * HALF, 16), HALF)

    def exists(v):
        return (v >= 0) & (v < 4 * STEPS) & (lax.rem(v, 2 * STEPS) != 2 * STEPS - 1)

    def packed(v):
        return v - jnp.where(v >= 2 * STEPS, 1, 0)

    def part_copy(v):
        w = packed(v)
        return pltpu.make_async_remote_copy(
            src_ref=OWN.at[lax.rem(v, KEEP), :, theirs, :],
            dst_ref=PART.at[w],
            send_sem=sem_d2d.at[lax.rem(v, 4)],
            recv_sem=sem_part.at[w],
            device_id=partner,
            device_id_type=MESH,
        )

    def up_copy(w):
        return pltpu.make_async_remote_copy(
            src_ref=OUT.at[lax.rem(w, SLOTS)],
            dst_ref=G.at[w, :, mine, :],
            send_sem=sem_out.at[lax.rem(w, SLOTS)],
            recv_sem=sem_up.at[w],
            device_id=at(onward, core),
            device_id_type=MESH,
        )

    def back_copy(w):
        return pltpu.make_async_remote_copy(
            src_ref=G.at[w, :, mine, :],
            dst_ref=G.at[w, :, mine, :],
            send_sem=sem_gsend.at[0],
            recv_sem=sem_g.at[w],
            device_id=at(back, core),
            device_id_type=MESH,
        )

    def share_copy(w):
        return pltpu.make_async_remote_copy(
            src_ref=G.at[w, :, mine, :],
            dst_ref=G.at[w, :, mine, :],
            send_sem=sem_share.at[0],
            recv_sem=sem_shared.at[0],
            device_id=partner,
            device_id_type=MESH,
        )

    def reduce(v):
        @pl.when(exists(v))
        def _():
            w = packed(v)
            slot = lax.rem(w, SLOTS)
            part_copy(v).wait_recv()

            def two(k):
                return OWN[lax.rem(v, KEEP), k, mine, :].astype(F32) + PART[w, k].astype(F32)

            @pl.when((w >= SLOTS) & (distance < 3))
            def _():
                up_copy(w).wait_send()

            @pl.when(distance == 0)
            def _():
                for k in range(3):
                    OUT[slot, k] = two(k).astype(BF16)

            @pl.when(distance > 0)
            def _():
                up_copy(w).wait_recv()

            @pl.when((distance > 0) & (distance < 3))
            def _():
                for k in range(3):
                    OUT[slot, k] = (two(k) + G[w, k, mine, :].astype(F32)).astype(BF16)

            @pl.when(distance < 3)
            def _():
                up_copy(w).start()

            @pl.when(distance == 3)
            def _():
                total = jnp.zeros((8, LANES), F32)
                for k in range(3):
                    g = (two(k) + G[w, k, mine, :].astype(F32)).astype(BF16)
                    G[w, k, mine, :] = g
                    g = g.astype(F32)
                    total += jnp.sum((g * g).reshape(HALF // 8, 8, LANES), 0)
                SQ[...] += total
                back_copy(w).start()
                share_copy(w).start()

    def gather(v):
        @pl.when(exists(v) & (distance < 3))
        def _():
            w = packed(v)
            back_copy(w).wait_recv()

            @pl.when(distance > 0)
            def _():
                back_copy(w).start()

            share_copy(w).start()

    def ss_copy(other):
        return pltpu.make_async_remote_copy(
            src_ref=SQ,
            dst_ref=SS.at[core],
            send_sem=sem_sssend.at[other],
            recv_sem=sem_ss.at[core],
            device_id=(rep, lax.rem(dp + other, 8)),
            device_id_type=MESH,
        )

    def communicate(n):
        reduce(n - FIRST - LAG * distance)
        gather(n - FIRST - LAG * 3 - BACK * (3 - distance))

    @pl.loop(0, 2 * STEPS)
    def _(t):
        q = t + STEPS
        slot = lax.rem(q, 2)

        @pl.when(t == STEPS)
        def _():
            next_layer()

        wait_tile(q)

        @pl.when(q < 3 * STEPS - 1)
        def _():
            load(q + 1)

        for r in range(0, T, ROWS):
            gu = dot(A[r : r + ROWS, :], WGU[slot])
            da = dot_t(DY[r : r + ROWS, :], WD[slot]).astype(BF16).astype(F32)
            g, u = gu[:, :TILE], gu[:, TILE:]
            sig = 0.5 * jnp.tanh(0.5 * g) + 0.5
            s = g * sig
            ACT[r : r + ROWS, :] = (s * u).astype(BF16)
            DT[r : r + ROWS, TILE:] = (da * s).astype(BF16)
            DT[r : r + ROWS, :TILE] = (da * u * (sig + s * (1.0 - sig))).astype(BF16)

        communicate(2 * t)

        keep = lax.rem(t, KEEP // 2) * 2
        dgu = dot(AT[...], DT[...]).astype(BF16)
        for k in range(2):
            for half in range(2):
                OWN[keep + half, k] = dgu[:, k * TILE + half * LANES : k * TILE + (half + 1) * LANES]
        dd = dot(DYT[...], ACT[...]).astype(BF16)
        for half in range(2):
            OWN[keep + half, 2] = dd[:, half * LANES : (half + 1) * LANES]

        for half in range(2):
            v = 2 * t + half

            @pl.when(exists(v - 2))
            def _():
                part_copy(v - 2).wait_send()

            @pl.when(exists(v))
            def _():
                part_copy(v).start()

        @pl.when(t == 0)
        def _():
            ACC[...] = jnp.zeros_like(ACC)

        @pl.when(t < STEPS)
        def _():
            for r in range(0, T, ROWS):
                ACC[r : r + ROWS, :] += dot_t(DT[r : r + ROWS, :], WGU[slot])

        communicate(2 * t + 1)

    part_copy(jnp.int32(4 * STEPS - 2)).wait_send()

    whole = pl.ds(0, AHEAD_UNITS * LANES)
    ahead = (
        pltpu.make_async_copy(wd_hbm.at[:, whole, :], XA, sem_ahead.at[0]),
        pltpu.make_async_copy(wg_hbm.at[:, :, whole], ATS, sem_ahead.at[1]),
        pltpu.make_async_copy(md_hbm.at[1, whole, :], ACC, sem_ahead.at[2]),
    )
    for copy in ahead:
        copy.start()

    def up_ahead(u, half):
        columns = pl.ds(pl.multiple_of(lax.rem(u, PER_LAYER) * LANES, LANES), LANES)
        rows = pl.ds(half * HALF, HALF)
        return pltpu.make_async_copy(wu_hbm.at[jnp.where(u < PER_LAYER, 1, 0), rows, columns], PART.at[u, half], sem_ahead.at[3])

    @pl.loop(4 * STEPS, LAST)
    def _(n):
        communicate(n)

        @pl.when(n >= SUMMED)
        def _():
            first = (n - SUMMED) * AT_A_TIME

            @pl.loop(first, jnp.minimum(first + AT_A_TIME, UNITS))
            def _(u):
                for half in range(2):
                    up_ahead(u, half).start()

        @pl.when((n == SUMMED) & (distance == 3))
        def _():
            for other in range(1, 8):
                ss_copy(other).start()
            SS[core] = SQ[...]

    @pl.when(distance < 3)
    def _():
        for w in range(UNITS - SLOTS, UNITS):
            up_copy(jnp.int32(w)).wait_send()

    everything = G.at[:, :, mine, :]
    others = G.at[:, :, theirs, :]

    @pl.when(distance > 0)
    def _():
        pltpu.make_async_copy(everything, everything, sem_gsend.at[0]).wait()

    pltpu.make_async_copy(everything, everything, sem_share.at[0]).wait()
    pltpu.make_async_copy(others, others, sem_shared.at[0]).wait()

    for copy in ahead:
        copy.wait()
    landed = PART.at[:, pl.ds(0, 2)]
    pltpu.make_async_copy(landed, landed, sem_ahead.at[3]).wait()

    for piece in range(2):

        @pl.when(jnp.logical_not((distance == 3) & (core == piece)))
        def _():
            pltpu.make_async_copy(SS.at[piece], SS.at[piece], sem_ss.at[piece]).wait()

    @pl.when(distance == 3)
    def _():
        for other in range(1, 8):
            ss_copy(other).wait_send()

    ss_out[...] = SS[0] + SS[1]


def gradients(x, dy, w_gate, w_up, w_down, m_down):
    hbm = pl.BlockSpec(memory_space=pl.ANY)

    def vmem(*shape):
        return pltpu.VMEM(shape, BF16)

    dma = pltpu.SemaphoreType.DMA
    return pl.pallas_call(
        gradient_kernel,
        out_shape=(
            vmem(UNITS, 3, D, LANES), pltpu.VMEM((8, LANES), F32),
            vmem(2, T, D), vmem(2, D, T), vmem(UNITS, 3, HALF, LANES), pltpu.VMEM((T, D), F32),
        ),
        in_specs=[hbm] * 6,
        out_specs=(pl.BlockSpec(memory_space=pltpu.VMEM),) * 6,
        scratch_shapes=[
            vmem(T, D), vmem(T, D),
            vmem(T, 2 * TILE), vmem(T, TILE), vmem(2, D, 2 * TILE), vmem(2, TILE, D),
            vmem(KEEP, 3, D, LANES), vmem(SLOTS, 3, HALF, LANES),
            pltpu.VMEM((8, LANES), F32), pltpu.VMEM((2, 8, LANES), F32), dma((4,)),
            dma((T // 256 + 1,)), dma((2, 3)), dma((4,)), dma((UNITS,)), dma((UNITS,)), dma((SLOTS,)),
            dma((UNITS,)), dma((1,)), dma((1,)), dma((1,)), dma((2,)), dma((8,)),
        ],
        compiler_params=pltpu.CompilerParams(collective_id=0, has_side_effects=True, vmem_limit_bytes=22 * 2**20),
        name="gradients",
    )(x, dy, w_gate, w_up, w_down, m_down)


def update(w, m, v, g):
    m = 0.9 * m + 0.1 * g
    v = 0.95 * v + 0.05 * g * g
    step = m * lax.rsqrt(v + 1e-8) + 0.1 * w
    return (w - 0.02 * step).astype(BF16), m, v


def clip_factor(ss_ref):
    total = jnp.sum(ss_ref[...], keepdims=True)
    return jnp.minimum(1.0, 0.5 * lax.rsqrt(total / (UNITS * 3 * D * LANES) + 1e-30))


def adamw_kernel(ss, g, w_down_ahead, w_gate_ahead, w_up_ahead, m_down_ahead, *refs):
    w_in, m_in, v_in, w_new, m_new, v_new = (refs[i : i + 3] for i in range(0, 18, 3))
    WI, MI, VI, WO, DWI, DMI, DVI, DWO, sem_in, sem_out = refs[18:]
    factor = clip_factor(ss)

    def place(k, u):
        columns = pl.ds(pl.multiple_of(lax.rem(u, PER_LAYER) * LANES, LANES), LANES)
        layer = jnp.where(u < PER_LAYER, 1, 0)
        return (layer, slice(None), columns) if k < 2 else (layer, columns, slice(None))

    def buffers(k, u):
        slot = lax.rem(u, DEEP)
        if k < 2:
            return tuple(ref.at[slot, k] for ref in (WI, MI, VI, WO))
        return tuple(ref.at[slot] for ref in (DWI, DMI, DVI, DWO))

    def reads(k, u):
        slot, at, (w, m, v, _) = lax.rem(u, DEEP), place(k, u), buffers(k, u)
        pairs = ((w_in[k].at[at], w), (m_in[k].at[at], m), (v_in[k].at[at], v))
        return [pltpu.make_async_copy(src, dst, sem_in.at[slot, k, i]) for i, (src, dst) in enumerate(pairs)]

    def is_ahead(u):
        return lax.rem(u, PER_LAYER) < AHEAD_UNITS

    def each_read(k, u, act):
        w, m, v = reads(k, u)
        act(v)
        if k == 2:
            pl.when(jnp.logical_not(is_ahead(u) & (u < PER_LAYER)))(lambda: act(m))
        else:
            act(m)
        if k != 1:
            pl.when(jnp.logical_not(is_ahead(u)))(lambda: act(w))

    def writes(k, u):
        slot, at, (_, m, v, w) = lax.rem(u, DEEP), place(k, u), buffers(k, u)
        pairs = ((w, w_new[k].at[at]), (m, m_new[k].at[at]), (v, v_new[k].at[at]))
        return [pltpu.make_async_copy(src, dst, sem_out.at[slot, k, i]) for i, (src, dst) in enumerate(pairs)]

    def start_reads(u):
        for k in range(3):
            each_read(k, u, lambda copy: copy.start())

    for u in range(AHEAD):
        start_reads(jnp.int32(u))

    @pl.loop(0, UNITS)
    def _(u):
        later = u + AHEAD

        @pl.when(later < UNITS)
        def _():
            @pl.when(later >= DEEP)
            def _():
                for k in range(3):
                    for copy in writes(k, later - DEEP):
                        copy.wait()

            start_reads(later)

        layer = jnp.where(u < PER_LAYER, 1, 0)
        columns = pl.ds(pl.multiple_of(lax.rem(u, PER_LAYER) * LANES, LANES), LANES)

        def new_values(k, old_w, old_m):
            w, m, v, out = buffers(k, u)
            step = 160 if k < 2 else LANES
            for r in range(0, D, step):
                piece = slice(r, r + step)
                gradient = g[u, k, piece, :]
                at = (piece, slice(None)) if k < 2 else (slice(None), piece)
                gradient = (gradient if k < 2 else gradient.T).astype(F32) * factor
                out[at], m[at], v[at] = update(old_w(r, at).astype(F32), old_m(at), v[at], gradient)

        def read_w(k):
            return lambda r, at: buffers(k, u)[0][at]

        def read_m(k):
            return lambda at: buffers(k, u)[1][at]

        def down_w(r, at):
            return w_down_ahead[layer, columns, at[1]]

        for k in range(3):
            each_read(k, u, lambda copy: copy.wait())
            if k == 0:
                pl.when(is_ahead(u))(lambda: new_values(0, lambda r, at: w_gate_ahead[layer, at[0], columns], read_m(0)))
                pl.when(jnp.logical_not(is_ahead(u)))(lambda: new_values(0, read_w(0), read_m(0)))
            elif k == 1:
                new_values(1, lambda r, at: w_up_ahead[u, r // HALF, r % HALF : r % HALF + 160, :], read_m(1))
            else:
                both = is_ahead(u) & (u < PER_LAYER)
                pl.when(both)(lambda: new_values(2, down_w, lambda at: m_down_ahead[columns, at[1]]))
                pl.when(is_ahead(u) & (u >= PER_LAYER))(lambda: new_values(2, down_w, read_m(2)))
                pl.when(jnp.logical_not(is_ahead(u)))(lambda: new_values(2, read_w(2), read_m(2)))
            for copy in writes(k, u):
                copy.start()

    for u in range(UNITS - DEEP, UNITS):
        for k in range(3):
            for copy in writes(k, jnp.int32(u)):
                copy.wait()


def adamw(ss, g, ahead, weights, m, v):
    hbm = pl.BlockSpec(memory_space=pltpu.HBM)
    near = [pltpu.with_memory_space_constraint(a, pltpu.VMEM) for a in (ss, g, *ahead)]
    dma = pltpu.SemaphoreType.DMA
    return pl.pallas_call(
        adamw_kernel,
        in_specs=[pl.BlockSpec(memory_space=pltpu.VMEM)] * 6 + [hbm] * 9,
        out_specs=(hbm,) * 9,
        out_shape=tuple(jax.ShapeDtypeStruct(a.shape, a.dtype) for a in (*weights, *m, *v)),
        scratch_shapes=[
            pltpu.VMEM((DEEP, 2, D, LANES), BF16), pltpu.VMEM((DEEP, 2, D, LANES), F32), pltpu.VMEM((DEEP, 2, D, LANES), F32),
            pltpu.VMEM((DEEP, 2, D, LANES), BF16),
            pltpu.VMEM((DEEP, LANES, D), BF16), pltpu.VMEM((DEEP, LANES, D), F32), pltpu.VMEM((DEEP, LANES, D), F32),
            pltpu.VMEM((DEEP, LANES, D), BF16), dma((DEEP, 3, 3)), dma((DEEP, 3, 3)),
        ],
        compiler_params=pltpu.CompilerParams(vmem_limit_bytes=22 * 2**20),
        name="adamw",
    )(*near, *weights, *m, *v)


def solution(mesh):
    def step(x, dy, *arrays):
        weights, m, v = (arrays[i : i + 3] for i in (0, 3, 6))
        g, ss, *ahead = gradients(x, dy, *weights, m[2])
        return adamw(ss, g, ahead, weights, m, v)

    return jax.shard_map(
        step,
        mesh=mesh,
        in_specs=(P(("rep", "dp"), None, None),) * 2 + (P(None, None, None),) * 9,
        out_specs=(P("rep", None, None),) * 9,
        check_vma=False,
    )
```

```python
import functools

import jax
import jax.numpy as jnp
from jax import lax
from jax.experimental import pallas as pl
from jax.experimental.pallas import tpu as pltpu
from jax.sharding import PartitionSpec as P

F32, BF16 = jnp.float32, jnp.bfloat16
MESH = pl.DeviceIdType.MESH
T, D, FF = 2048, 640, 2432
TILE = 256
STEPS = 10
LANES = 128
PER_LAYER = FF // LANES
UNITS = 2 * PER_LAYER
ROWS, FORWARD_ROWS = 512, 1024
HALF = D // 2
KEEP = 10
SLOTS = 4
FIRST = 1
LAG = 2
BACK = 2
SUMMED = 2 * 2 * STEPS + FIRST + 3 * LAG
LAST = SUMMED + 3 * BACK
AT_A_TIME = -(-UNITS // (LAST - SUMMED))

DEEP, AHEAD = 7, 4
AHEAD_UNITS = T // LANES


def dot(a, b):
    return jnp.dot(a, b, preferred_element_type=F32)


def dot_t(a, b):
    return lax.dot_general(a, b, (((1,), (1,)), ((), ())), preferred_element_type=F32)


def norm_scale(h):
    wide = h.astype(F32)
    return wide, lax.rsqrt(jnp.mean(wide * wide, -1, keepdims=True) + 1e-6)


def gradient_kernel(
    x_hbm, dy_hbm, wg_hbm, wu_hbm, wd_hbm, md_hbm, G, ss_out, XA, ATS, PART, ACC,
    H, DY, DT, ACT, WGU, WD, OWN, OUT, SQ, SS, sem_ahead,
    sem_in, sem_w, sem_d2d, sem_part, sem_up, sem_out, sem_g, sem_gsend, sem_share, sem_shared, sem_ss, sem_sssend,
):
    X, A, AT, DYT = XA.at[0], XA.at[1], ATS.at[0], ATS.at[1]
    rep, dp = lax.axis_index("rep"), lax.axis_index("dp")
    z, core = lax.div(dp, 2), lax.rem(dp, 2)

    def at(z, core):
        return (rep, z * 2 + core)

    partner = at(z, 1 - core)
    barrier = pltpu.get_barrier_semaphore()
    for other in range(1, 8):
        pl.semaphore_signal(barrier, inc=1, device_id=(rep, lax.rem(dp + other, 8)), device_id_type=MESH)

    block = 256

    def rows_of(r):
        return pl.ds(pl.multiple_of(r * block, block), block)

    def x_copy(r):
        return pltpu.make_async_copy(x_hbm.at[0, rows_of(r), :], X.at[rows_of(r), :], sem_in.at[r])

    dy_copy = pltpu.make_async_copy(dy_hbm.at[0], DY, sem_in.at[T // block])
    for r in range(T // block):
        x_copy(jnp.int32(r)).start()

    def tile_copies(q, n):
        layer = jnp.where((q >= STEPS) & (q < 2 * STEPS), 1, 0)
        slot = lax.rem(q, 2)
        columns = pl.ds(pl.multiple_of(lax.rem(q, STEPS) * TILE, LANES), n)
        return (
            pltpu.make_async_copy(wg_hbm.at[layer, :, columns], WGU.at[slot, :, pl.ds(0, n)], sem_w.at[slot, 0]),
            pltpu.make_async_copy(wu_hbm.at[layer, :, columns], WGU.at[slot, :, pl.ds(TILE, n)], sem_w.at[slot, 1]),
            pltpu.make_async_copy(wd_hbm.at[layer, columns, :], WD.at[slot, pl.ds(0, n), :], sem_w.at[slot, 2]),
        )

    def load(q):
        short = lax.rem(q, STEPS) == STEPS - 1
        slot = lax.rem(q, 2)

        @pl.when(jnp.logical_not(short))
        def _():
            for copy in tile_copies(q, TILE):
                copy.start()

        @pl.when(short)
        def _():
            WGU[slot, :, LANES:TILE] = jnp.zeros((D, LANES), BF16)
            WGU[slot, :, TILE + LANES :] = jnp.zeros((D, LANES), BF16)
            WD[slot, LANES:, :] = jnp.zeros((LANES, D), BF16)
            for copy in tile_copies(q, LANES):
                copy.start()

    def wait_tile(q):
        short = lax.rem(q, STEPS) == STEPS - 1

        @pl.when(jnp.logical_not(short))
        def _():
            for copy in tile_copies(q, TILE):
                copy.wait()

        @pl.when(short)
        def _():
            for copy in tile_copies(q, LANES):
                copy.wait()

    load(jnp.int32(0))
    dy_copy.start()

    @pl.loop(0, T // block)
    def _(r):
        x_copy(r).wait()
        rows = rows_of(r)
        wide, scale = norm_scale(X[rows, :])
        A[rows, :] = (wide * scale).astype(BF16)

    def forward(q, first):
        slot = lax.rem(q, 2)
        wait_tile(q)
        load(q + 1)
        for r in range(0, T, FORWARD_ROWS):
            gu = dot(A[r : r + FORWARD_ROWS, :], WGU[slot])
            g, u = gu[:, :TILE], gu[:, TILE:]
            sig = 0.5 * jnp.tanh(0.5 * g) + 0.5
            h = dot((g * sig * u).astype(BF16), WD[slot])
            if first:
                ACC[r : r + FORWARD_ROWS, :] = h
            else:
                ACC[r : r + FORWARD_ROWS, :] += h
        if not first:
            rows = rows_of(jnp.minimum(q - 1, T // block - 1))
            DYT[:, rows] = DY[rows, :].T

    forward(jnp.int32(0), True)
    dy_copy.wait()

    @pl.loop(1, STEPS)
    def _(q):
        forward(q, False)

    @pl.loop(0, T // block)
    def _(r):
        rows = rows_of(r)
        h = (X[rows, :].astype(F32) + ACC[rows, :].astype(BF16).astype(F32)).astype(BF16)
        H[rows, :] = h
        wide, scale = norm_scale(h)
        a = (wide * scale).astype(BF16)
        A[rows, :] = a
        AT[:, rows] = a.T

    pl.semaphore_wait(barrier, 7)

    def next_layer():
        @pl.loop(0, T // block)
        def _(r):
            rows = rows_of(r)
            h, scale = norm_scale(H[rows, :])
            da = ACC[rows, :].astype(BF16).astype(F32)
            along = jnp.mean(da * h, -1, keepdims=True) * scale * scale
            dh = (scale * (da - h * along)).astype(BF16)
            d = (DY[rows, :].astype(F32) + dh.astype(F32)).astype(BF16)
            DY[rows, :] = d
            DYT[:, rows] = d.T
            wide, scale = norm_scale(X[rows, :])
            a = (wide * scale).astype(BF16)
            A[rows, :] = a
            AT[:, rows] = a.T

    SQ[...] = jnp.zeros_like(SQ)
    distance = jnp.where(core == 0, 3 - z, z)
    onward = jnp.where(core == 0, jnp.maximum(z - 1, 0), jnp.minimum(z + 1, 3))
    back = jnp.where(core == 0, jnp.minimum(z + 1, 3), jnp.maximum(z - 1, 0))
    mine = pl.ds(pl.multiple_of(core * HALF, 16), HALF)
    theirs = pl.ds(pl.multiple_of((1 - core) * HALF, 16), HALF)

    def exists(v):
        return (v >= 0) & (v < 4 * STEPS) & (lax.rem(v, 2 * STEPS) != 2 * STEPS - 1)

    def packed(v):
        return v - jnp.where(v >= 2 * STEPS, 1, 0)

    def part_copy(v):
        w = packed(v)
        return pltpu.make_async_remote_copy(
            src_ref=OWN.at[lax.rem(v, KEEP), :, theirs, :],
            dst_ref=PART.at[w],
            send_sem=sem_d2d.at[lax.rem(v, 4)],
            recv_sem=sem_part.at[w],
            device_id=partner,
            device_id_type=MESH,
        )

    def up_copy(w):
        return pltpu.make_async_remote_copy(
            src_ref=OUT.at[lax.rem(w, SLOTS)],
            dst_ref=G.at[w, :, mine, :],
            send_sem=sem_out.at[lax.rem(w, SLOTS)],
            recv_sem=sem_up.at[w],
            device_id=at(onward, core),
            device_id_type=MESH,
        )

    def back_copy(w):
        return pltpu.make_async_remote_copy(
            src_ref=G.at[w, :, mine, :],
            dst_ref=G.at[w, :, mine, :],
            send_sem=sem_gsend.at[0],
            recv_sem=sem_g.at[w],
            device_id=at(back, core),
            device_id_type=MESH,
        )

    def share_copy(w):
        return pltpu.make_async_remote_copy(
            src_ref=G.at[w, :, mine, :],
            dst_ref=G.at[w, :, mine, :],
            send_sem=sem_share.at[0],
            recv_sem=sem_shared.at[0],
            device_id=partner,
            device_id_type=MESH,
        )

    def reduce(v):
        @pl.when(exists(v))
        def _():
            w = packed(v)
            slot = lax.rem(w, SLOTS)
            part_copy(v).wait_recv()

            def two(k):
                return OWN[lax.rem(v, KEEP), k, mine, :].astype(F32) + PART[w, k].astype(F32)

            @pl.when((w >= SLOTS) & (distance < 3))
            def _():
                up_copy(w).wait_send()

            @pl.when(distance == 0)
            def _():
                for k in range(3):
                    OUT[slot, k] = two(k).astype(BF16)

            @pl.when(distance > 0)
            def _():
                up_copy(w).wait_recv()

            @pl.when((distance > 0) & (distance < 3))
            def _():
                for k in range(3):
                    OUT[slot, k] = (two(k) + G[w, k, mine, :].astype(F32)).astype(BF16)

            @pl.when(distance < 3)
            def _():
                up_copy(w).start()

            @pl.when(distance == 3)
            def _():
                total = jnp.zeros((8, LANES), F32)
                for k in range(3):
                    g = (two(k) + G[w, k, mine, :].astype(F32)).astype(BF16)
                    G[w, k, mine, :] = g
                    g = g.astype(F32)
                    total += jnp.sum((g * g).reshape(HALF // 8, 8, LANES), 0)
                SQ[...] += total
                back_copy(w).start()
                share_copy(w).start()

    def gather(v):
        @pl.when(exists(v) & (distance < 3))
        def _():
            w = packed(v)
            back_copy(w).wait_recv()

            @pl.when(distance > 0)
            def _():
                back_copy(w).start()

            share_copy(w).start()

    def ss_copy(other):
        return pltpu.make_async_remote_copy(
            src_ref=SQ,
            dst_ref=SS.at[core],
            send_sem=sem_sssend.at[other],
            recv_sem=sem_ss.at[core],
            device_id=(rep, lax.rem(dp + other, 8)),
            device_id_type=MESH,
        )

    def communicate(n):
        reduce(n - FIRST - LAG * distance)
        gather(n - FIRST - LAG * 3 - BACK * (3 - distance))

    @pl.loop(0, 2 * STEPS)
    def _(t):
        q = t + STEPS
        slot = lax.rem(q, 2)

        @pl.when(t == STEPS)
        def _():
            next_layer()

        wait_tile(q)

        @pl.when(q < 3 * STEPS - 1)
        def _():
            load(q + 1)

        for r in range(0, T, ROWS):
            gu = dot(A[r : r + ROWS, :], WGU[slot])
            da = dot_t(DY[r : r + ROWS, :], WD[slot]).astype(BF16).astype(F32)
            g, u = gu[:, :TILE], gu[:, TILE:]
            sig = 0.5 * jnp.tanh(0.5 * g) + 0.5
            s = g * sig
            ACT[r : r + ROWS, :] = (s * u).astype(BF16)
            DT[r : r + ROWS, TILE:] = (da * s).astype(BF16)
            DT[r : r + ROWS, :TILE] = (da * u * (sig + s * (1.0 - sig))).astype(BF16)

        communicate(2 * t)

        keep = lax.rem(t, KEEP // 2) * 2
        dgu = dot(AT[...], DT[...]).astype(BF16)
        for k in range(2):
            for half in range(2):
                OWN[keep + half, k] = dgu[:, k * TILE + half * LANES : k * TILE + (half + 1) * LANES]
        dd = dot(DYT[...], ACT[...]).astype(BF16)
        for half in range(2):
            OWN[keep + half, 2] = dd[:, half * LANES : (half + 1) * LANES]

        for half in range(2):
            v = 2 * t + half

            @pl.when(exists(v - 2))
            def _():
                part_copy(v - 2).wait_send()

            @pl.when(exists(v))
            def _():
                part_copy(v).start()

        @pl.when(t == 0)
        def _():
            ACC[...] = jnp.zeros_like(ACC)

        @pl.when(t < STEPS)
        def _():
            for r in range(0, T, ROWS):
                ACC[r : r + ROWS, :] += dot_t(DT[r : r + ROWS, :], WGU[slot])

        communicate(2 * t + 1)

    part_copy(jnp.int32(4 * STEPS - 2)).wait_send()

    whole = pl.ds(0, AHEAD_UNITS * LANES)
    ahead = (
        pltpu.make_async_copy(wd_hbm.at[:, whole, :], XA, sem_ahead.at[0]),
        pltpu.make_async_copy(wg_hbm.at[:, :, whole], ATS, sem_ahead.at[1]),
        pltpu.make_async_copy(md_hbm.at[1, whole, :], ACC, sem_ahead.at[2]),
    )
    for copy in ahead:
        copy.start()

    def up_ahead(u, half):
        columns = pl.ds(pl.multiple_of(lax.rem(u, PER_LAYER) * LANES, LANES), LANES)
        rows = pl.ds(half * HALF, HALF)
        return pltpu.make_async_copy(wu_hbm.at[jnp.where(u < PER_LAYER, 1, 0), rows, columns], PART.at[u, half], sem_ahead.at[3])

    @pl.loop(4 * STEPS, LAST)
    def _(n):
        communicate(n)

        @pl.when(n >= SUMMED)
        def _():
            first = (n - SUMMED) * AT_A_TIME

            @pl.loop(first, jnp.minimum(first + AT_A_TIME, UNITS))
            def _(u):
                for half in range(2):
                    up_ahead(u, half).start()

        @pl.when((n == SUMMED) & (distance == 3))
        def _():
            for other in range(1, 8):
                ss_copy(other).start()
            SS[core] = SQ[...]

    @pl.when(distance < 3)
    def _():
        for w in range(UNITS - SLOTS, UNITS):
            up_copy(jnp.int32(w)).wait_send()

    everything = G.at[:, :, mine, :]
    others = G.at[:, :, theirs, :]

    @pl.when(distance > 0)
    def _():
        pltpu.make_async_copy(everything, everything, sem_gsend.at[0]).wait()

    pltpu.make_async_copy(everything, everything, sem_share.at[0]).wait()
    pltpu.make_async_copy(others, others, sem_shared.at[0]).wait()

    for copy in ahead:
        copy.wait()
    landed = PART.at[:, pl.ds(0, 2)]
    pltpu.make_async_copy(landed, landed, sem_ahead.at[3]).wait()

    for piece in range(2):

        @pl.when(jnp.logical_not((distance == 3) & (core == piece)))
        def _():
            pltpu.make_async_copy(SS.at[piece], SS.at[piece], sem_ss.at[piece]).wait()

    @pl.when(distance == 3)
    def _():
        for other in range(1, 8):
            ss_copy(other).wait_send()

    ss_out[...] = SS[0] + SS[1]


def gradients(x, dy, w_gate, w_up, w_down, m_down):
    hbm = pl.BlockSpec(memory_space=pl.ANY)

    def vmem(*shape):
        return pltpu.VMEM(shape, BF16)

    dma = pltpu.SemaphoreType.DMA
    return pl.pallas_call(
        gradient_kernel,
        out_shape=(
            vmem(UNITS, 3, D, LANES), pltpu.VMEM((8, LANES), F32),
            vmem(2, T, D), vmem(2, D, T), vmem(UNITS, 3, HALF, LANES), pltpu.VMEM((T, D), F32),
        ),
        in_specs=[hbm] * 6,
        out_specs=(pl.BlockSpec(memory_space=pltpu.VMEM),) * 6,
        scratch_shapes=[
            vmem(T, D), vmem(T, D),
            vmem(T, 2 * TILE), vmem(T, TILE), vmem(2, D, 2 * TILE), vmem(2, TILE, D),
            vmem(KEEP, 3, D, LANES), vmem(SLOTS, 3, HALF, LANES),
            pltpu.VMEM((8, LANES), F32), pltpu.VMEM((2, 8, LANES), F32), dma((4,)),
            dma((T // 256 + 1,)), dma((2, 3)), dma((4,)), dma((UNITS,)), dma((UNITS,)), dma((SLOTS,)),
            dma((UNITS,)), dma((1,)), dma((1,)), dma((1,)), dma((2,)), dma((8,)),
        ],
        compiler_params=pltpu.CompilerParams(collective_id=0, has_side_effects=True, vmem_limit_bytes=22 * 2**20),
        name="gradients",
    )(x, dy, w_gate, w_up, w_down, m_down)


def update(w, m, v, g):
    m = 0.9 * m + 0.1 * g
    v = 0.95 * v + 0.05 * g * g
    step = m * lax.rsqrt(v + 1e-8) + 0.1 * w
    return (w - 0.02 * step).astype(BF16), m, v


def clip_factor(ss_ref):
    total = jnp.sum(ss_ref[...], keepdims=True)
    return jnp.minimum(1.0, 0.5 * lax.rsqrt(total / (UNITS * 3 * D * LANES) + 1e-30))


def adamw_kernel(ss, g, w_down_ahead, w_gate_ahead, w_up_ahead, m_down_ahead, *refs):
    w_in, m_in, v_in, w_new, m_new, v_new = (refs[i : i + 3] for i in range(0, 18, 3))
    WI, MI, VI, WO, DWI, DMI, DVI, DWO, sem_in, sem_out = refs[18:]
    factor = clip_factor(ss)

    def place(k, u):
        columns = pl.ds(pl.multiple_of(lax.rem(u, PER_LAYER) * LANES, LANES), LANES)
        layer = jnp.where(u < PER_LAYER, 1, 0)
        return (layer, slice(None), columns) if k < 2 else (layer, columns, slice(None))

    def buffers(k, u):
        slot = lax.rem(u, DEEP)
        if k < 2:
            return tuple(ref.at[slot, k] for ref in (WI, MI, VI, WO))
        return tuple(ref.at[slot] for ref in (DWI, DMI, DVI, DWO))

    def reads(k, u):
        slot, at, (w, m, v, _) = lax.rem(u, DEEP), place(k, u), buffers(k, u)
        pairs = ((w_in[k].at[at], w), (m_in[k].at[at], m), (v_in[k].at[at], v))
        return [pltpu.make_async_copy(src, dst, sem_in.at[slot, k, i]) for i, (src, dst) in enumerate(pairs)]

    def is_ahead(u):
        return lax.rem(u, PER_LAYER) < AHEAD_UNITS

    def each_read(k, u, act):
        w, m, v = reads(k, u)
        act(v)
        if k == 2:
            pl.when(jnp.logical_not(is_ahead(u) & (u < PER_LAYER)))(lambda: act(m))
        else:
            act(m)
        if k != 1:
            pl.when(jnp.logical_not(is_ahead(u)))(lambda: act(w))

    def writes(k, u):
        slot, at, (_, m, v, w) = lax.rem(u, DEEP), place(k, u), buffers(k, u)
        pairs = ((w, w_new[k].at[at]), (m, m_new[k].at[at]), (v, v_new[k].at[at]))
        return [pltpu.make_async_copy(src, dst, sem_out.at[slot, k, i]) for i, (src, dst) in enumerate(pairs)]

    def start_reads(u):
        for k in range(3):
            each_read(k, u, lambda copy: copy.start())

    for u in range(AHEAD):
        start_reads(jnp.int32(u))

    @pl.loop(0, UNITS)
    def _(u):
        later = u + AHEAD

        @pl.when(later < UNITS)
        def _():
            @pl.when(later >= DEEP)
            def _():
                for k in range(3):
                    for copy in writes(k, later - DEEP):
                        copy.wait()

            start_reads(later)

        layer = jnp.where(u < PER_LAYER, 1, 0)
        columns = pl.ds(pl.multiple_of(lax.rem(u, PER_LAYER) * LANES, LANES), LANES)

        def new_values(k, old_w, old_m):
            w, m, v, out = buffers(k, u)
            step = 160 if k < 2 else LANES
            for r in range(0, D, step):
                piece = slice(r, r + step)
                gradient = g[u, k, piece, :]
                at = (piece, slice(None)) if k < 2 else (slice(None), piece)
                gradient = (gradient if k < 2 else gradient.T).astype(F32) * factor
                out[at], m[at], v[at] = update(old_w(r, at).astype(F32), old_m(at), v[at], gradient)

        def read_w(k):
            return lambda r, at: buffers(k, u)[0][at]

        def read_m(k):
            return lambda at: buffers(k, u)[1][at]

        def down_w(r, at):
            return w_down_ahead[layer, columns, at[1]]

        for k in range(3):
            each_read(k, u, lambda copy: copy.wait())
            if k == 0:
                pl.when(is_ahead(u))(lambda: new_values(0, lambda r, at: w_gate_ahead[layer, at[0], columns], read_m(0)))
                pl.when(jnp.logical_not(is_ahead(u)))(lambda: new_values(0, read_w(0), read_m(0)))
            elif k == 1:
                new_values(1, lambda r, at: w_up_ahead[u, r // HALF, r % HALF : r % HALF + 160, :], read_m(1))
            else:
                both = is_ahead(u) & (u < PER_LAYER)
                pl.when(both)(lambda: new_values(2, down_w, lambda at: m_down_ahead[columns, at[1]]))
                pl.when(is_ahead(u) & (u >= PER_LAYER))(lambda: new_values(2, down_w, read_m(2)))
                pl.when(jnp.logical_not(is_ahead(u)))(lambda: new_values(2, read_w(2), read_m(2)))
            for copy in writes(k, u):
                copy.start()

    for u in range(UNITS - DEEP, UNITS):
        for k in range(3):
            for copy in writes(k, jnp.int32(u)):
                copy.wait()


def adamw(ss, g, ahead, weights, m, v):
    hbm = pl.BlockSpec(memory_space=pltpu.HBM)
    near = [pltpu.with_memory_space_constraint(a, pltpu.VMEM) for a in (ss, g, *ahead)]
    dma = pltpu.SemaphoreType.DMA
    return pl.pallas_call(
        adamw_kernel,
        in_specs=[pl.BlockSpec(memory_space=pltpu.VMEM)] * 6 + [hbm] * 9,
        out_specs=(hbm,) * 9,
        out_shape=tuple(jax.ShapeDtypeStruct(a.shape, a.dtype) for a in (*weights, *m, *v)),
        scratch_shapes=[
            pltpu.VMEM((DEEP, 2, D, LANES), BF16), pltpu.VMEM((DEEP, 2, D, LANES), F32), pltpu.VMEM((DEEP, 2, D, LANES), F32),
            pltpu.VMEM((DEEP, 2, D, LANES), BF16),
            pltpu.VMEM((DEEP, LANES, D), BF16), pltpu.VMEM((DEEP, LANES, D), F32), pltpu.VMEM((DEEP, LANES, D), F32),
            pltpu.VMEM((DEEP, LANES, D), BF16), dma((DEEP, 3, 3)), dma((DEEP, 3, 3)),
        ],
        compiler_params=pltpu.CompilerParams(vmem_limit_bytes=22 * 2**20),
        name="adamw",
    )(*near, *weights, *m, *v)


def solution(mesh):
    def step(x, dy, *arrays):
        weights, m, v = (arrays[i : i + 3] for i in (0, 3, 6))
        g, ss, *ahead = gradients(x, dy, *weights, m[2])
        return adamw(ss, g, ahead, weights, m, v)

    return jax.shard_map(
        step,
        mesh=mesh,
        in_specs=(P(("rep", "dp"), None, None),) * 2 + (P(None, None, None),) * 9,
        out_specs=(P("rep", None, None),) * 9,
        check_vma=False,
    )
```
